32 devices in a mesh: sector: 8 (over y, x, core), row: 4 (over z).
Axes of the slice: x: 2, y: 2, z: 4, core: 2. Of those that a mesh axis runs over, the one named last changes fastest.
Arguments:
- psi_sectors: bfloat16 [32, 8192, 256], P('sector', 'row'), may hold values from -1.5 to 1.5
- stiff_blocks: bfloat16 [64, 5, 128, 128], P('row'), as said below
- mass_blocks: bfloat16 [64, 5, 128, 128], P('row'), as said below
- harmonic_table: int32 [16], replicated, may hold values from 0 to 15, each once
Outputs:
- reduced_stiffness: float32 [16, 512, 512], P('sector', 'row')
- reduced_mass: float32 [16, 512, 512], P('sector', 'row')
The draws below stay inside these ranges and needn't reach their ends.
Inputs may be any that keep to these rules, and one draw needn't show every extreme that they name: The stiffness is symmetric: stiff_blocks[i, 2 + d] is the transpose of stiff_blocks[i + d, 2 - d], and blocks whose column lies outside 0 to 63 are zero. `mass_blocks`: the mass is symmetric in the same way, and diagonally dominant with a positive diagonal, hence positive definite.
All inputs are finite; a program needn't handle non-finite values.
Results may differ from the reference program's by a relative error of at most 0.0049.
Values may be sent and summed in bfloat16 or wider, within the bound.
A program may use at most 128 MiB of HBM per device.

```python
import math
import jax
import jax.numpy as jnp
from jax import lax

M = 256
B = 128
REACH = 2
NBAND = 5
SECTORS = 32
SLOTS = 16
DOF = 8192
NBLK = 64


def build_band(key, entry_scale):
    upper_part = jnp.clip(jax.random.normal(key, (NBLK, REACH + 1, B, B), jnp.float32), -6.0, 6.0) * entry_scale
    middle = (upper_part[:, 0] + jnp.swapaxes(upper_part[:, 0], 1, 2)) * 0.5 ** 0.5
    block_ids = jnp.arange(NBLK, dtype=jnp.int32)[:, None, None]
    columns = []
    for offset in range(-REACH, REACH + 1):
        if offset == 0:
            columns.append(middle)
        elif offset > 0:
            inside = block_ids + offset < NBLK
            columns.append(jnp.where(inside, upper_part[:, offset], 0.0))
        else:
            distance = -offset
            flipped = jnp.swapaxes(upper_part[:, distance], 1, 2)
            shifted = jnp.concatenate([jnp.zeros((distance, B, B), jnp.float32), flipped[:NBLK - distance]], axis=0)
            columns.append(shifted)
    return jnp.stack(columns, axis=1)


def draw_stiff_blocks(key, part):
    band = build_band(jax.random.fold_in(key, 11), (NBAND * B) ** (-0.5))
    return band.astype(jnp.bfloat16)


def draw_mass_blocks(key, part):
    band = build_band(jax.random.fold_in(key, 23), 1.0 / (NBAND * B))
    identity = jnp.eye(B, dtype=jnp.float32)
    own_diagonal = jnp.abs(jnp.diagonal(band[:, REACH], axis1=1, axis2=2))
    off_sum = jnp.sum(jnp.abs(band), axis=(1, 3)) - own_diagonal
    factor = jax.random.uniform(jax.random.fold_in(key, 29), (NBLK, B), jnp.float32, 1.1, 2.0)
    new_diagonal = off_sum * factor
    centre = band[:, REACH] * (1.0 - identity) + new_diagonal[:, :, None] * identity
    band = band.at[:, REACH].set(centre)
    return band.astype(jnp.bfloat16)


def block_scale(key, dims, cuts, smallest, largest):
    level = 1.0
    for position, parts in cuts:
        steps = jax.random.uniform(jax.random.fold_in(jax.random.fold_in(key, 6), position), (parts,), jnp.float32, smallest / len(cuts), largest / len(cuts))
        level = level * jnp.repeat(jnp.exp(steps), dims[position] // parts).reshape((-1,) + (1,) * (len(dims) - 1 - position))
    return level


def gaussian(rng, extent, spread, reach, split=(), kind=jnp.bfloat16):
    entries = jax.random.normal(rng, extent, jnp.float32) * spread
    if len(split) > 0:
        entries = block_scale(rng, extent, split, -0.22, 0.18) * entries
    return jnp.clip(entries, min=-reach, max=reach).astype(kind)


def setup_inputs(seed: int = 0) -> dict:
    streams_of = jax.random.split(jax.random.key(seed), 5)
    return {
        "psi_sectors": gaussian(streams_of[0], (SECTORS, DOF, M), (DOF ** -0.25), 1.5, ((0, 8), (1, 4))),
        "stiff_blocks": draw_stiff_blocks(jax.random.fold_in(streams_of[4], 71), 0),
        "mass_blocks": draw_mass_blocks(jax.random.fold_in(streams_of[4], 71), 0),
        "harmonic_table": jax.random.permutation(streams_of[3], SLOTS).astype(jnp.int32),
    }


def coefficients(harmonic_table, sectors_all):
    sector_ids = jnp.arange(sectors_all, dtype=jnp.int32)
    pair_table = harmonic_table.astype(jnp.int32)
    half_count = sectors_all // 2
    second_freq = jnp.where(pair_table == 0, half_count, pair_table)
    first_phase = pair_table[:, None] * sector_ids[None, :] % sectors_all
    second_phase = second_freq[:, None] * sector_ids[None, :] % sectors_all
    angle_unit = 2.0 * math.pi / sectors_all
    first_angle = first_phase.astype(jnp.float32) * angle_unit
    second_angle = second_phase.astype(jnp.float32) * angle_unit
    zero_pair = (pair_table == 0)[:, None]
    low_scale = math.sqrt(1.0 / sectors_all)
    high_scale = math.sqrt(2.0 / sectors_all)
    first_row = jnp.where(zero_pair, low_scale, high_scale) * jnp.cos(first_angle)
    second = jnp.where(zero_pair, low_scale * jnp.cos(second_angle), high_scale * jnp.sin(second_angle))
    return jnp.stack([first_row, second], axis=1).reshape(2 * pair_table.shape[0], sectors_all)

def band_apply(blocks, harmonic):
    block_rows = blocks.shape[0]
    band_count = blocks.shape[1]
    padded = jnp.pad(harmonic.reshape(block_rows, B, harmonic.shape[1]), ((REACH, REACH), (0, 0), (0, 0)))
    block_index = jnp.arange(block_rows, dtype=jnp.int32)[:, None] + jnp.arange(band_count, dtype=jnp.int32)[None, :]
    gathered = padded[block_index].astype(jnp.float32)
    images = jnp.einsum('ijab,ijbm->iam', blocks.astype(jnp.float32), gathered)
    return images.reshape(harmonic.shape).astype(jnp.bfloat16)

def reference(psi_sectors, stiff_blocks, mass_blocks, harmonic_table):
    sectors_all = psi_sectors.shape[0]
    dof_count = psi_sectors.shape[1]
    mode_count = psi_sectors.shape[2]
    dft_table = coefficients(harmonic_table, sectors_all)
    flattened = psi_sectors.reshape(sectors_all, dof_count * mode_count).astype(jnp.float32)
    harmonics = jnp.dot(dft_table, flattened, precision=lax.Precision.HIGHEST).astype(jnp.bfloat16)
    harmonics = harmonics.reshape(sectors_all // 2, 2, dof_count, mode_count)

    def one_slot(pair_field):
        left_basis = jnp.concatenate([pair_field[0], pair_field[1]], axis=1)
        stiff_wide = jnp.concatenate([band_apply(stiff_blocks, pair_field[0]), band_apply(stiff_blocks, pair_field[1])], axis=1)
        mass_wide = jnp.concatenate([band_apply(mass_blocks, pair_field[0]), band_apply(mass_blocks, pair_field[1])], axis=1)
        return (jnp.dot(left_basis.T, stiff_wide, preferred_element_type=jnp.float32), jnp.dot(left_basis.T, mass_wide, preferred_element_type=jnp.float32))
    reduced_stiffness, reduced_mass = lax.map(one_slot, harmonics)
    return (reduced_stiffness, reduced_mass)
```

```python
import functools
import math

import jax
import jax.numpy as jnp
from jax import lax
from jax.experimental import pallas as pl
from jax.experimental.pallas import tpu as pltpu
from jax.sharding import PartitionSpec as P

MESH = pl.DeviceIdType.MESH
LANES = 128
PACK = 16
CHUNKS = 4


def flipped(index, step, count):
    total, bit = 0, 1
    while bit < count:
        total = total + bit * lax.rem(lax.div(index, bit) + (step // bit) % 2, 2)
        bit *= 2
    return total


def kernel(cfg, table_ref, psi_ref, stiff_ref, mass_ref, out_k, out_m,
           x_buf, h_buf, p_buf, pt_buf, y_buf, band, g_part, g_send, g_recv, f_send, f_row, f_col, weights,
           s1, r1, s2, r2, sh, rh, s3, r3, sf, rf, lb):
    n, zn, sec, rows, modes, nblk, nband, blk = cfg
    slots = sec // 2
    part = rows // n
    chunk = part // CHUNKS
    reach = nband // 2
    halo = reach * blk
    total = 2 * modes
    own_rows = total // zn
    halves = modes // LANES
    cols = total // LANES
    groups = slots * cols
    turn = [cols - 1 - c // 2 if c % 2 else c // 2 for c in range(cols)]
    share = zn // cols
    root = [turn[c] * share for c in range(cols)]
    tri = [c * (c + 1) // 2 for c in range(cols)]
    wide = 2 * LANES
    sectors_all = n * sec
    d = lax.axis_index("sector")
    z = lax.axis_index("row")
    order = [j for j in (2, 4, 6, 3, 5, 7) if j < n] + [1]
    order += [j for j in range(1, n) if j not in order]

    barrier = pltpu.get_barrier_semaphore()
    for j in order:
        pl.semaphore_signal(barrier, inc=1, device_id={"sector": flipped(d, j, n)}, device_id_type=MESH)
    for j in range(1, zn):
        pl.semaphore_signal(barrier, inc=1, device_id={"row": lax.rem(z + j, zn)}, device_id_type=MESH)
    pl.semaphore_wait(barrier, n - 1 + zn - 1)

    def settle(ref, sem, what):
        getattr(pltpu.make_async_remote_copy(
            src_ref=ref, dst_ref=ref, send_sem=sem, recv_sem=sem,
            device_id={"row": z}, device_id_type=MESH), what)()

    def first(q, j):
        target = flipped(d, j, n)
        return pltpu.make_async_remote_copy(
            src_ref=psi_ref.at[:, pl.ds(target * part + q * chunk, chunk), :],
            dst_ref=x_buf.at[q, pl.ds(d * sec, sec)],
            send_sem=s1.at[0], recv_sem=r1.at[q],
            device_id={"sector": target}, device_id_type=MESH)

    def first_own(q):
        return pltpu.make_async_copy(
            psi_ref.at[:, pl.ds(d * part + q * chunk, chunk), :],
            x_buf.at[q, pl.ds(d * sec, sec)], r1.at[q])

    def early(g, q, j):
        target = flipped(d, j, n)
        return pltpu.make_async_remote_copy(
            src_ref=h_buf.at[g, target, pl.ds(q * chunk, chunk), :],
            dst_ref=p_buf.at[g, pl.ds(halo + d * part + q * chunk, chunk), :],
            send_sem=s2.at[0], recv_sem=r2.at[g],
            device_id={"sector": target}, device_id_type=MESH)

    def second(g, j):
        target = flipped(d, j, n)
        return pltpu.make_async_remote_copy(
            src_ref=h_buf.at[g, target],
            dst_ref=p_buf.at[g, pl.ds(halo + d * part, part), :],
            send_sem=s2.at[0], recv_sem=r2.at[g],
            device_id={"sector": target}, device_id_type=MESH)

    def edge(g, up):
        source = rows if up else halo
        dest = 0 if up else halo + rows
        target = lax.rem(z + (1 if up else zn - 1), zn)
        return pltpu.make_async_remote_copy(
            src_ref=p_buf.at[g, pl.ds(source, halo), :],
            dst_ref=p_buf.at[g, pl.ds(dest, halo), :],
            send_sem=sh.at[int(up)], recv_sem=rh.at[g, int(up)],
            device_id={"row": target}, device_id_type=MESH)

    @pl.loop(0, CHUNKS)
    def _(q):
        for j in order:
            first(q, j).start()
        first_own(q).start()

    band_copies = [pltpu.make_async_copy(stiff_ref, band.at[0], lb.at[0]),
                   pltpu.make_async_copy(mass_ref, band.at[1], lb.at[1])]
    for copy in band_copies:
        copy.start()

    @pl.when(z == 0)
    def _():
        @pl.loop(0, groups)
        def _(g):
            p_buf[g, pl.ds(0, halo), :] = jnp.zeros((halo, LANES), p_buf.dtype)

    @pl.when(z == zn - 1)
    def _():
        @pl.loop(0, groups)
        def _(g):
            p_buf[g, pl.ds(halo + rows, halo), :] = jnp.zeros((halo, LANES), p_buf.dtype)

    wide_rows, wide_cols = 2 * n * PACK, sectors_all * PACK

    def spread(shape, long):
        return ((lax.broadcasted_iota(jnp.int32, shape, long) >> 4) == lax.broadcasted_iota(
            jnp.int32, shape, 1 - long)).astype(jnp.float32).astype(jnp.bfloat16)

    spread_rows = spread((wide_rows, LANES), 0)
    spread_cols = spread((LANES, wide_cols), 1)
    same = ((lax.broadcasted_iota(jnp.int32, (wide_rows, wide_cols), 0) & (PACK - 1))
            == (lax.broadcasted_iota(jnp.int32, (wide_rows, wide_cols), 1) & (PACK - 1)))
    line = lax.broadcasted_iota(jnp.int32, (LANES, LANES), 0)
    sector = lax.broadcasted_iota(jnp.int32, (LANES, LANES), 1)
    for h in range(slots):
        pair = jnp.zeros((LANES, LANES), jnp.int32)
        for e in range(n):
            pair = jnp.where((line == e) | (line == n + e), table_ref[e * slots + h], pair)
        lone = pair == 0
        upper = line >= n
        turns = jnp.where(lone & upper, sectors_all // 2, pair) * sector
        turns = turns + jnp.where(upper & jnp.logical_not(lone), sectors_all - sectors_all // 4, 0)
        turns = turns & (sectors_all - 1)
        scale = jnp.where(lone, math.sqrt(1.0 / sectors_all), math.sqrt(2.0 / sectors_all))
        value = scale * jnp.cos(turns.astype(jnp.float32) * (2.0 * math.pi / sectors_all))
        high = value.astype(jnp.bfloat16)
        low = (value - high.astype(jnp.float32)).astype(jnp.bfloat16)
        for index, piece in enumerate((high, low)):
            tall = jnp.dot(spread_rows, piece, preferred_element_type=jnp.float32).astype(jnp.bfloat16)
            full = jnp.dot(tall, spread_cols, preferred_element_type=jnp.float32)
            weights[h, index] = jnp.where(same, full, 0.0).astype(jnp.bfloat16)

    @pl.loop(0, CHUNKS)
    def _(q):
        settle(x_buf.at[q], r1.at[q], "wait_recv")

        @pl.loop(0, chunk // PACK)
        def _(t):
            x = x_buf[q, :, pl.ds(pl.multiple_of(t * PACK, PACK), PACK), :].reshape(wide_cols, modes)
            at = pl.ds(pl.multiple_of(q * chunk + t * PACK, PACK), PACK)
            for h in range(slots):
                value = (jnp.dot(weights[h, 0], x, preferred_element_type=jnp.float32)
                         + jnp.dot(weights[h, 1], x, preferred_element_type=jnp.float32)).astype(jnp.bfloat16)
                for c in range(cols):
                    k, half = turn[c] // halves, turn[c] % halves
                    h_buf[h * cols + c, :, at, :] = value[
                        k * n * PACK:(k + 1) * n * PACK, half * LANES:(half + 1) * LANES].reshape(n, PACK, LANES)

        for g in range(halves):
            for j in order:
                early(g, q, j).start()

    @pl.loop(halves, groups)
    def _(g):
        for j in order:
            second(g, j).start()

    @pl.loop(0, groups)
    def _(g):
        p_buf[g, pl.ds(pl.multiple_of(halo + d * part, part), part), :] = h_buf[g, d]

    for copy in band_copies:
        copy.wait()

    def block_row(g, c, i):
        at = pl.ds(pl.multiple_of(i * blk, blk), blk)
        blocks = jnp.concatenate(
            [jnp.concatenate([band[which, i, k] for k in range(nband)], axis=1) for which in range(2)], axis=0)
        window = p_buf[g, pl.ds(pl.multiple_of(i * blk, blk), nband * blk), :]
        image = jnp.dot(blocks, window, preferred_element_type=jnp.float32).astype(jnp.bfloat16)
        y_buf[at, :LANES] = image[:blk]
        y_buf[at, LANES:] = image[blk:]
        pt_buf[c * LANES:(c + 1) * LANES, at] = window[halo:halo + blk].T

    def gram(h, c):
        value = jnp.dot(pt_buf[:(c + 1) * LANES, :], y_buf[...], preferred_element_type=jnp.float32)
        for b in range(c + 1):
            g_part[h, tri[c] + b] = value[b * LANES:(b + 1) * LANES]

    def relay(h, c, at, step):
        side = 0 if step > 0 else 1

        @pl.loop(0, c + 1)
        def _(b):
            value = g_part[h, tri[c] + b]
            if at not in (0, zn - 1):
                settle(g_recv.at[side, h, tri[c] + b], r3.at[side, h, tri[c] + b], "wait_recv")
                value = value + g_recv[side, h, tri[c] + b].astype(jnp.float32)
            g_send[h, tri[c] + b] = value.astype(jnp.bfloat16)
            pltpu.make_async_remote_copy(
                src_ref=g_send.at[h, tri[c] + b], dst_ref=g_recv.at[side, h, tri[c] + b],
                send_sem=s3.at[c], recv_sem=r3.at[side, h, tri[c] + b],
                device_id={"row": at + step}, device_id_type=MESH).start()

    def row_send(h, b, c, i):
        return pltpu.make_async_remote_copy(
            src_ref=f_send.at[h, tri[c] + b, pl.ds(i * own_rows, own_rows)], dst_ref=f_row.at[h, c],
            send_sem=sf.at[0, i], recv_sem=rf.at[0, h, c],
            device_id={"row": turn[b] * share + i}, device_id_type=MESH)

    def col_send(h, b, c, i):
        return pltpu.make_async_remote_copy(
            src_ref=f_send.at[h, tri[c] + b], dst_ref=f_col.at[h, b],
            send_sem=sf.at[1, i], recv_sem=rf.at[1, h, b],
            device_id={"row": root[c] + i}, device_id_type=MESH)

    def close(h, c):
        for b in range(c + 1):
            value = g_part[h, tri[c] + b]
            for side, present in ((0, root[c] > 0), (1, root[c] < zn - 1)):
                if present:
                    settle(g_recv.at[side, h, tri[c] + b], r3.at[side, h, tri[c] + b], "wait_recv")
                    value = value + g_recv[side, h, tri[c] + b].astype(jnp.float32)
            if b < c or share > 1:
                f_send[h, tri[c] + b] = value.astype(jnp.bfloat16)
            for i in range(share):
                if b < c or i > 0:
                    row_send(h, b, c, i).start()
                if b < c and i > 0:
                    col_send(h, b, c, i).start()
            if b < c:
                keep_across(h, b, value, 0)
            else:
                keep_rows(h, c, value[:own_rows])

    def keep_rows(h, c, value):
        span = slice(turn[c] * LANES, (turn[c] + 1) * LANES)
        out_k[h, :, span] = value[:, :LANES]
        out_m[h, :, span] = value[:, LANES:]

    def keep_across(h, b, value, i):
        span = slice(turn[b] * LANES, (turn[b] + 1) * LANES)
        own = slice(i * own_rows, (i + 1) * own_rows)
        out_k[h, :, span] = value[:, :LANES].T[own]
        out_m[h, :, span] = value[:, LANES:].T[own]

    def advance(h, c, p):
        if p < root[c]:
            pl.when(z == p)(lambda: relay(h, c, p, 1))
        if zn - 1 - p > root[c]:
            pl.when(z == zn - 1 - p)(lambda: relay(h, c, zn - 1 - p, -1))
        if p == max(root[c], zn - 1 - root[c]):
            pl.when(z == root[c])(lambda: close(h, c))

    def take(g):
        settle(h_buf.at[g, pl.ds(0, n - 1)], r2.at[g], "wait_recv")

        @pl.when(z < zn - 1)
        def _():
            edge(g, True).start()

        @pl.when(z > 0)
        def _():
            edge(g, False).start()

    @pl.loop(0, slots)
    def _(h):
        for c in range(cols):
            g = h * cols + c
            take(g)

            @pl.loop(reach, nblk - reach)
            def _(i):
                block_row(g, c, i)

            for p in range(zn - 1, 0, -1):
                older = (c - p) // cols
                if older == 0:
                    advance(h, (c - p) % cols, p)
                else:
                    @pl.when(h + older >= 0)
                    def _():
                        advance(h + older, (c - p) % cols, p)

            @pl.when(z > 0)
            def _():
                edge(g, True).wait_recv()

            @pl.when(z < zn - 1)
            def _():
                edge(g, False).wait_recv()

            @pl.loop(0, 2 * reach)
            def _(i):
                block_row(g, c, lax.rem(i + nblk - reach, nblk))

            gram(h, c)
            advance(h, c, 0)

    for t in range(1, zn):
        for p in range(zn - 1, t - 1, -1):
            late = groups - 1 + t - p
            if late >= 0:
                advance(late // cols, late % cols, p)

    for c in range(cols):
        for b in range(c + 1):
            for i in range(share):
                if b < c or i > 0:
                    @pl.when(z == turn[b] * share + i)
                    def _():
                        for h in range(slots):
                            settle(f_row.at[h, c], rf.at[0, h, c], "wait_recv")
                            keep_rows(h, c, f_row[h, c].astype(jnp.float32))
                if b < c and i > 0:
                    @pl.when(z == root[c] + i)
                    def _():
                        for h in range(slots):
                            settle(f_col.at[h, b], rf.at[1, h, b], "wait_recv")
                            keep_across(h, b, f_col[h, b].astype(jnp.float32), i)

    settle(psi_ref.at[:, pl.ds(0, (n - 1) * part), :], s1.at[0], "wait_send")
    settle(h_buf.at[:, pl.ds(0, n - 1)], s2.at[0], "wait_send")

    @pl.when(z < zn - 1)
    def _():
        settle(p_buf.at[:, pl.ds(0, halo), :], sh.at[1], "wait_send")

    @pl.when(z > 0)
    def _():
        settle(p_buf.at[:, pl.ds(0, halo), :], sh.at[0], "wait_send")

    for c in range(cols):
        @pl.when(z != root[c])
        def _():
            settle(g_send.at[:, pl.ds(tri[c], c + 1)], s3.at[c], "wait_send")

        @pl.when(z == root[c])
        def _():
            for i in range(share):
                count = c + 1 if i > 0 else c
                if count > 0:
                    settle(f_send.at[:, pl.ds(0, count), pl.ds(0, own_rows)], sf.at[0, i], "wait_send")
                if c > 0 and i > 0:
                    settle(f_send.at[:, pl.ds(0, c)], sf.at[1, i], "wait_send")


def flush(a_ref, b_ref, a_out, b_out, sem):
    copies = [pltpu.make_async_copy(a_ref, a_out, sem.at[0]), pltpu.make_async_copy(b_ref, b_out, sem.at[1])]
    for copy in copies:
        copy.start()
    for copy in copies:
        copy.wait()


def per_device(psi_sectors, stiff_blocks, mass_blocks, harmonic_table):
    sec, rows, modes = psi_sectors.shape
    nblk, nband, blk, _ = stiff_blocks.shape
    n, zn = lax.axis_size("sector"), lax.axis_size("row")
    sectors_all = sec * n
    slots = sec // 2
    part = rows // n
    chunk = part // CHUNKS
    halo = (nband // 2) * blk
    total = 2 * modes
    cols = total // LANES
    own_rows = total // zn
    bf16, f32 = jnp.bfloat16, jnp.float32
    dma = pltpu.SemaphoreType.DMA
    vmem = pl.BlockSpec(memory_space=pltpu.VMEM)
    hbm = pl.BlockSpec(memory_space=pl.ANY)
    share = zn // cols
    tiles = cols * (cols + 1) // 2
    wide = 2 * LANES
    held = pltpu.VMEM((slots, own_rows, total), f32)
    final = jax.ShapeDtypeStruct((slots, own_rows, total), f32)
    stiff, mass = pl.pallas_call(
        functools.partial(kernel, (n, zn, sec, rows, modes, nblk, nband, blk)),
        out_shape=(held, held),
        in_specs=[pl.BlockSpec(memory_space=pltpu.SMEM), hbm, hbm, hbm],
        out_specs=(vmem, vmem),
        scratch_shapes=[
            pltpu.VMEM((CHUNKS, sectors_all, chunk, modes), bf16),
            pltpu.VMEM((slots * cols, n, part, LANES), bf16),
            pltpu.VMEM((slots * cols, rows + 2 * halo, LANES), bf16),
            pltpu.VMEM((total, rows), bf16),
            pltpu.VMEM((rows, wide), bf16),
            pltpu.VMEM((2, nblk, nband, blk, blk), bf16),
            pltpu.VMEM((slots, tiles, LANES, wide), f32),
            pltpu.VMEM((slots, tiles, LANES, wide), bf16),
            pltpu.VMEM((2, slots, tiles, LANES, wide), bf16),
            pltpu.VMEM((slots, tiles, LANES, wide), bf16),
            pltpu.VMEM((slots, cols, own_rows, wide), bf16),
            pltpu.VMEM((slots, cols, LANES, wide), bf16),
            pltpu.VMEM((slots, 2, 2 * n * PACK, sectors_all * PACK), bf16),
            dma((1,)), dma((CHUNKS,)),
            dma((1,)), dma((slots * cols,)),
            dma((2,)), dma((slots * cols, 2)),
            dma((cols,)), dma((2, slots, tiles)),
            dma((2, share)), dma((2, slots, cols)),
            dma((2,)),
        ],
        compiler_params=pltpu.CompilerParams(
            collective_id=0, has_side_effects=True, vmem_limit_bytes=60000 * 1024),
    )(harmonic_table, psi_sectors, stiff_blocks, mass_blocks)
    return pl.pallas_call(
        flush, out_shape=(final, final), in_specs=[vmem, vmem], out_specs=(hbm, hbm),
        scratch_shapes=[dma((2,))], compiler_params=pltpu.CompilerParams(vmem_limit_bytes=1024 * 1024),
    )(stiff, mass)


def solution(mesh):
    placed = (P("sector", "row", None), P("row", None, None, None), P("row", None, None, None), P())
    return jax.shard_map(
        per_device,
        mesh=mesh,
        in_specs=placed,
        out_specs=(P("sector", "row", None), P("sector", "row", None)),
        check_vma=False,
    )
```

```python
import functools
import math

import jax
import jax.numpy as jnp
from jax import lax
from jax.experimental import pallas as pl
from jax.experimental.pallas import tpu as pltpu
from jax.sharding import PartitionSpec as P

MESH = pl.DeviceIdType.MESH
LANES = 128
PACK = 16
CHUNKS = 4
LEAD = 2


def flipped(index, step, count):
    total, bit = 0, 1
    while bit < count:
        total = total + bit * lax.rem(lax.div(index, bit) + (step // bit) % 2, 2)
        bit *= 2
    return total


def kernel(cfg, table_ref, psi_ref, stiff_ref, mass_ref, out_k, out_m,
           x_buf, h_buf, p_buf, pt_buf, y_buf, band, g_part, g_send, g_recv, f_send, f_row, f_col, weights,
           s1, r1, s2, r2, re, sh, rh, s3, r3, sf, rf, lb):
    n, zn, sec, rows, modes, nblk, nband, blk = cfg
    slots = sec // 2
    part = rows // n
    chunk = part // CHUNKS
    reach = nband // 2
    halo = reach * blk
    rim = halo // n
    inner = part - 2 * rim
    total = 2 * modes
    own_rows = total // zn
    halves = modes // LANES
    cols = total // LANES
    groups = slots * cols
    turn = [cols - 1 - c // 2 if c % 2 else c // 2 for c in range(cols)]
    share = zn // cols
    root = [turn[c] * share for c in range(cols)]
    tri = [c * (c + 1) // 2 for c in range(cols)]
    wide = 2 * LANES
    sectors_all = n * sec
    d = lax.axis_index("sector")
    z = lax.axis_index("row")
    order = [j for j in (2, 4, 6, 3, 5, 7) if j < n] + [1]
    order += [j for j in range(1, n) if j not in order]

    barrier = pltpu.get_barrier_semaphore()
    for j in order:
        pl.semaphore_signal(barrier, inc=1, device_id={"sector": flipped(d, j, n)}, device_id_type=MESH)
    for j in range(1, zn):
        pl.semaphore_signal(barrier, inc=1, device_id={"row": lax.rem(z + j, zn)}, device_id_type=MESH)
    pl.semaphore_wait(barrier, n - 1 + zn - 1)

    def settle(ref, sem, what):
        getattr(pltpu.make_async_remote_copy(
            src_ref=ref, dst_ref=ref, send_sem=sem, recv_sem=sem,
            device_id={"row": z}, device_id_type=MESH), what)()

    def rim_low(device):
        return pl.multiple_of(device * rim, rim)

    def rim_high(device):
        return pl.multiple_of(rows - halo + device * rim, rim)

    def middle(device, q):
        return pl.multiple_of(halo + device * inner + (q - 1) * chunk, chunk)

    def first_parts(device, q):
        if isinstance(q, int) and q == 0:
            return [(rim_low(device), 0, rim), (rim_high(device), rim, rim)]
        return [(middle(device, q), 0, chunk)]

    def first(q, j):
        target = flipped(d, j, n)
        return [pltpu.make_async_remote_copy(
            src_ref=psi_ref.at[:, pl.ds(start, count), :],
            dst_ref=x_buf.at[q, pl.ds(d * sec, sec), pl.ds(at, count), :],
            send_sem=s1.at[0], recv_sem=r1.at[q],
            device_id={"sector": target}, device_id_type=MESH) for start, at, count in first_parts(target, q)]

    def first_own(q):
        return [pltpu.make_async_copy(
            psi_ref.at[:, pl.ds(start, count), :],
            x_buf.at[q, pl.ds(d * sec, sec), pl.ds(at, count), :], r1.at[q])
            for start, at, count in first_parts(d, q)]

    partner = flipped(d, 1, n)

    def towards(core):
        return [2 * lax.div(flipped(d, j, n), 2) + core for j in order if j % 2 == 0]

    def rims(g, target):
        for start, at in ((rim_low(d), 0), (rim_high(d), rim)):
            pltpu.make_async_remote_copy(
                src_ref=h_buf.at[g, target, pl.ds(at, rim), :],
                dst_ref=p_buf.at[g, pl.ds(halo + start, rim), :],
                send_sem=s2.at[0], recv_sem=re.at[g],
                device_id={"sector": target}, device_id_type=MESH).start()

    def second(g, target, q=None):
        at, count = (2 * rim, inner) if q is None else (pl.multiple_of(2 * rim + (q - 1) * chunk, chunk), chunk)
        pltpu.make_async_remote_copy(
            src_ref=h_buf.at[g, target, pl.ds(at, count), :],
            dst_ref=p_buf.at[g, pl.ds(halo + middle(d, 1 if q is None else q), count), :],
            send_sem=s2.at[0], recv_sem=r2.at[g],
            device_id={"sector": target}, device_id_type=MESH).start()

    def edges(g):
        settle(h_buf.at[g, pl.ds(0, n - 1), pl.ds(0, 2 * rim)], re.at[g], "wait_recv")

        @pl.when(z < zn - 1)
        def _():
            edge(g, True).start()

        @pl.when(z > 0)
        def _():
            edge(g, False).start()

    def edge(g, up):
        source = rows if up else halo
        dest = 0 if up else halo + rows
        target = lax.rem(z + (1 if up else zn - 1), zn)
        return pltpu.make_async_remote_copy(
            src_ref=p_buf.at[g, pl.ds(source, halo), :],
            dst_ref=p_buf.at[g, pl.ds(dest, halo), :],
            send_sem=sh.at[int(up)], recv_sem=rh.at[g, int(up)],
            device_id={"row": target}, device_id_type=MESH)

    def first_start(q):
        for j in order:
            for copy in first(q, j):
                copy.start()
        for copy in first_own(q):
            copy.start()

    first_start(0)
    first_start(1)

    band_copies = [pltpu.make_async_copy(stiff_ref, band.at[0], lb.at[0]),
                   pltpu.make_async_copy(mass_ref, band.at[1], lb.at[1])]
    for copy in band_copies:
        copy.start()

    @pl.when(z == 0)
    def _():
        @pl.loop(0, groups)
        def _(g):
            p_buf[g, pl.ds(0, halo), :] = jnp.zeros((halo, LANES), p_buf.dtype)

    @pl.when(z == zn - 1)
    def _():
        @pl.loop(0, groups)
        def _(g):
            p_buf[g, pl.ds(halo + rows, halo), :] = jnp.zeros((halo, LANES), p_buf.dtype)

    wide_rows, wide_cols = 2 * n * PACK, sectors_all * PACK

    def spread(shape, long):
        return ((lax.broadcasted_iota(jnp.int32, shape, long) >> 4) == lax.broadcasted_iota(
            jnp.int32, shape, 1 - long)).astype(jnp.float32).astype(jnp.bfloat16)

    spread_rows = spread((wide_rows, LANES), 0)
    spread_cols = spread((LANES, wide_cols), 1)
    same = ((lax.broadcasted_iota(jnp.int32, (wide_rows, wide_cols), 0) & (PACK - 1))
            == (lax.broadcasted_iota(jnp.int32, (wide_rows, wide_cols), 1) & (PACK - 1)))
    line = lax.broadcasted_iota(jnp.int32, (LANES, LANES), 0)
    sector = lax.broadcasted_iota(jnp.int32, (LANES, LANES), 1)
    for h in range(slots):
        pair = jnp.zeros((LANES, LANES), jnp.int32)
        for e in range(n):
            pair = jnp.where((line == e) | (line == n + e), table_ref[e * slots + h], pair)
        lone = pair == 0
        upper = line >= n
        turns = jnp.where(lone & upper, sectors_all // 2, pair) * sector
        turns = turns + jnp.where(upper & jnp.logical_not(lone), sectors_all - sectors_all // 4, 0)
        turns = turns & (sectors_all - 1)
        scale = jnp.where(lone, math.sqrt(1.0 / sectors_all), math.sqrt(2.0 / sectors_all))
        value = scale * jnp.cos(turns.astype(jnp.float32) * (2.0 * math.pi / sectors_all))
        high = value.astype(jnp.bfloat16)
        low = (value - high.astype(jnp.float32)).astype(jnp.bfloat16)
        for index, piece in enumerate((high, low)):
            tall = jnp.dot(spread_rows, piece, preferred_element_type=jnp.float32).astype(jnp.bfloat16)
            full = jnp.dot(tall, spread_cols, preferred_element_type=jnp.float32)
            weights[h, index] = jnp.where(same, full, 0.0).astype(jnp.bfloat16)

    def transform(q):
        settle(x_buf.at[q], r1.at[q], "wait_recv")

        @pl.loop(0, chunk // PACK)
        def _(t):
            x = x_buf[q, :, pl.ds(pl.multiple_of(t * PACK, PACK), PACK), :].reshape(wide_cols, modes)
            at = pl.ds(pl.multiple_of(q * chunk + t * PACK, PACK), PACK)
            for h in range(slots):
                value = (jnp.dot(weights[h, 0], x, preferred_element_type=jnp.float32)
                         + jnp.dot(weights[h, 1], x, preferred_element_type=jnp.float32)).astype(jnp.bfloat16)
                for c in range(cols):
                    k, half = turn[c] // halves, turn[c] % halves
                    h_buf[h * cols + c, :, at, :] = value[
                        k * n * PACK:(k + 1) * n * PACK, half * LANES:(half + 1) * LANES].reshape(n, PACK, LANES)

    everyone = towards(0) + towards(1) + [partner]
    transform(0)
    for g in range(LEAD):
        for target in everyone:
            rims(g, target)

    @pl.loop(2, CHUNKS)
    def _(q):
        first_start(q)

    @pl.loop(0, groups)
    def _(g):
        p_buf[g, pl.ds(halo + rim_low(d), rim), :] = h_buf[g, d, pl.ds(0, rim)]
        p_buf[g, pl.ds(halo + rim_high(d), rim), :] = h_buf[g, d, pl.ds(rim, rim)]

    def middle_chunk(q):
        transform(q)
        for target in everyone:
            second(0, target, q)

    middle_chunk(1)
    for g in range(LEAD):
        edges(g)

    @pl.loop(2, CHUNKS)
    def _(q):
        middle_chunk(q)

    for target in everyone:
        rims(LEAD, target)

    @pl.loop(1, groups)
    def _(g):
        for targets in ([partner], towards(0), towards(1)):
            for target in targets:
                second(g, target)

            @pl.when(g + LEAD < groups)
            def _():
                for target in targets:
                    rims(g + LEAD, target)

    @pl.loop(0, groups)
    def _(g):
        p_buf[g, pl.ds(halo + middle(d, 1), inner), :] = h_buf[g, d, pl.ds(2 * rim, inner)]

    for copy in band_copies:
        copy.wait()

    def block_row(g, c, i):
        at = pl.ds(pl.multiple_of(i * blk, blk), blk)
        blocks = jnp.concatenate(
            [jnp.concatenate([band[which, i, k] for k in range(nband)], axis=1) for which in range(2)], axis=0)
        window = p_buf[g, pl.ds(pl.multiple_of(i * blk, blk), nband * blk), :]
        image = jnp.dot(blocks, window, preferred_element_type=jnp.float32).astype(jnp.bfloat16)
        y_buf[at, :LANES] = image[:blk]
        y_buf[at, LANES:] = image[blk:]
        pt_buf[c * LANES:(c + 1) * LANES, at] = window[halo:halo + blk].T

    def gram(h, c):
        value = jnp.dot(pt_buf[:(c + 1) * LANES, :], y_buf[...], preferred_element_type=jnp.float32)
        for b in range(c + 1):
            g_part[h, tri[c] + b] = value[b * LANES:(b + 1) * LANES]

    def relay(h, c, at, step):
        side = 0 if step > 0 else 1

        @pl.loop(0, c + 1)
        def _(b):
            value = g_part[h, tri[c] + b]
            if at not in (0, zn - 1):
                settle(g_recv.at[side, h, tri[c] + b], r3.at[side, h, tri[c] + b], "wait_recv")
                value = value + g_recv[side, h, tri[c] + b].astype(jnp.float32)
            g_send[h, tri[c] + b] = value.astype(jnp.bfloat16)
            pltpu.make_async_remote_copy(
                src_ref=g_send.at[h, tri[c] + b], dst_ref=g_recv.at[side, h, tri[c] + b],
                send_sem=s3.at[c], recv_sem=r3.at[side, h, tri[c] + b],
                device_id={"row": at + step}, device_id_type=MESH).start()

    def row_send(h, b, c, i):
        return pltpu.make_async_remote_copy(
            src_ref=f_send.at[h, tri[c] + b, pl.ds(i * own_rows, own_rows)], dst_ref=f_row.at[h, c],
            send_sem=sf.at[0, i], recv_sem=rf.at[0, h, c],
            device_id={"row": turn[b] * share + i}, device_id_type=MESH)

    def col_send(h, b, c, i):
        return pltpu.make_async_remote_copy(
            src_ref=f_send.at[h, tri[c] + b], dst_ref=f_col.at[h, b],
            send_sem=sf.at[1, i], recv_sem=rf.at[1, h, b],
            device_id={"row": root[c] + i}, device_id_type=MESH)

    def close(h, c):
        for b in range(c + 1):
            value = g_part[h, tri[c] + b]
            for side, present in ((0, root[c] > 0), (1, root[c] < zn - 1)):
                if present:
                    settle(g_recv.at[side, h, tri[c] + b], r3.at[side, h, tri[c] + b], "wait_recv")
                    value = value + g_recv[side, h, tri[c] + b].astype(jnp.float32)
            if b < c or share > 1:
                f_send[h, tri[c] + b] = value.astype(jnp.bfloat16)
            for i in range(share):
                if b < c or i > 0:
                    row_send(h, b, c, i).start()
                if b < c and i > 0:
                    col_send(h, b, c, i).start()
            if b < c:
                keep_across(h, b, value, 0)
            else:
                keep_rows(h, c, value[:own_rows])

    def keep_rows(h, c, value):
        span = slice(turn[c] * LANES, (turn[c] + 1) * LANES)
        out_k[h, :, span] = value[:, :LANES]
        out_m[h, :, span] = value[:, LANES:]

    def keep_across(h, b, value, i):
        span = slice(turn[b] * LANES, (turn[b] + 1) * LANES)
        own = slice(i * own_rows, (i + 1) * own_rows)
        out_k[h, :, span] = value[:, :LANES].T[own]
        out_m[h, :, span] = value[:, LANES:].T[own]

    def forward(h, c, p):
        if p < root[c]:
            pl.when(z == p)(lambda: relay(h, c, p, 1))
        if zn - 1 - p > root[c]:
            pl.when(z == zn - 1 - p)(lambda: relay(h, c, zn - 1 - p, -1))

    def settled(h, c, p):
        if p == max(root[c], zn - 1 - root[c]):
            pl.when(z == root[c])(lambda: close(h, c))

    @pl.loop(0, slots)
    def _(h):
        for c in range(cols):
            g = h * cols + c
            settle(h_buf.at[g, pl.ds(0, n - 1), pl.ds(0, inner)], r2.at[g], "wait_recv")

            @pl.when((g + 1 >= LEAD) & (g + 1 < groups))
            def _():
                edges(g + 1)

            @pl.when(z > 0)
            def _():
                edge(g, True).wait_recv()

            @pl.when(z < zn - 1)
            def _():
                edge(g, False).wait_recv()

            @pl.loop(0, nblk, unroll=4)
            def _(i):
                block_row(g, c, i)

            gram(h, c)
            forward(h, c, 0)

            for stage in (forward, settled):
                for p in range(zn - 1, 0, -1):
                    older = (c - p) // cols
                    if older == 0:
                        stage(h, (c - p) % cols, p)
                    else:
                        @pl.when(h + older >= 0)
                        def _():
                            stage(h + older, (c - p) % cols, p)

    for t in range(1, zn):
        for stage in (forward, settled):
            for p in range(zn - 1, t - 1, -1):
                late = groups - 1 + t - p
                if late >= 0:
                    stage(late // cols, late % cols, p)

    for c in range(cols):
        for b in range(c + 1):
            for i in range(share):
                if b < c or i > 0:
                    @pl.when(z == turn[b] * share + i)
                    def _():
                        for h in range(slots):
                            settle(f_row.at[h, c], rf.at[0, h, c], "wait_recv")
                            keep_rows(h, c, f_row[h, c].astype(jnp.float32))
                if b < c and i > 0:
                    @pl.when(z == root[c] + i)
                    def _():
                        for h in range(slots):
                            settle(f_col.at[h, b], rf.at[1, h, b], "wait_recv")
                            keep_across(h, b, f_col[h, b].astype(jnp.float32), i)

    settle(psi_ref.at[:, pl.ds(0, (n - 1) * part), :], s1.at[0], "wait_send")
    settle(h_buf.at[:, pl.ds(0, n - 1)], s2.at[0], "wait_send")

    @pl.when(z < zn - 1)
    def _():
        settle(p_buf.at[:, pl.ds(0, halo), :], sh.at[1], "wait_send")

    @pl.when(z > 0)
    def _():
        settle(p_buf.at[:, pl.ds(0, halo), :], sh.at[0], "wait_send")

    for c in range(cols):
        @pl.when(z != root[c])
        def _():
            settle(g_send.at[:, pl.ds(tri[c], c + 1)], s3.at[c], "wait_send")

        @pl.when(z == root[c])
        def _():
            for i in range(share):
                count = c + 1 if i > 0 else c
                if count > 0:
                    settle(f_send.at[:, pl.ds(0, count), pl.ds(0, own_rows)], sf.at[0, i], "wait_send")
                if c > 0 and i > 0:
                    settle(f_send.at[:, pl.ds(0, c)], sf.at[1, i], "wait_send")


def flush(a_ref, b_ref, a_out, b_out, sem):
    copies = [pltpu.make_async_copy(a_ref, a_out, sem.at[0]), pltpu.make_async_copy(b_ref, b_out, sem.at[1])]
    for copy in copies:
        copy.start()
    for copy in copies:
        copy.wait()


def per_device(psi_sectors, stiff_blocks, mass_blocks, harmonic_table):
    sec, rows, modes = psi_sectors.shape
    nblk, nband, blk, _ = stiff_blocks.shape
    n, zn = lax.axis_size("sector"), lax.axis_size("row")
    sectors_all = sec * n
    slots = sec // 2
    part = rows // n
    chunk = part // CHUNKS
    halo = (nband // 2) * blk
    total = 2 * modes
    cols = total // LANES
    own_rows = total // zn
    bf16, f32 = jnp.bfloat16, jnp.float32
    dma = pltpu.SemaphoreType.DMA
    vmem = pl.BlockSpec(memory_space=pltpu.VMEM)
    hbm = pl.BlockSpec(memory_space=pl.ANY)
    share = zn // cols
    tiles = cols * (cols + 1) // 2
    wide = 2 * LANES
    held = pltpu.VMEM((slots, own_rows, total), f32)
    final = jax.ShapeDtypeStruct((slots, own_rows, total), f32)
    stiff, mass = pl.pallas_call(
        functools.partial(kernel, (n, zn, sec, rows, modes, nblk, nband, blk)),
        out_shape=(held, held),
        in_specs=[pl.BlockSpec(memory_space=pltpu.SMEM), hbm, hbm, hbm],
        out_specs=(vmem, vmem),
        scratch_shapes=[
            pltpu.VMEM((CHUNKS, sectors_all, chunk, modes), bf16),
            pltpu.VMEM((slots * cols, n, part, LANES), bf16),
            pltpu.VMEM((slots * cols, rows + 2 * halo, LANES), bf16),
            pltpu.VMEM((total, rows), bf16),
            pltpu.VMEM((rows, wide), bf16),
            pltpu.VMEM((2, nblk, nband, blk, blk), bf16),
            pltpu.VMEM((slots, tiles, LANES, wide), f32),
            pltpu.VMEM((slots, tiles, LANES, wide), bf16),
            pltpu.VMEM((2, slots, tiles, LANES, wide), bf16),
            pltpu.VMEM((slots, tiles, LANES, wide), bf16),
            pltpu.VMEM((slots, cols, own_rows, wide), bf16),
            pltpu.VMEM((slots, cols, LANES, wide), bf16),
            pltpu.VMEM((slots, 2, 2 * n * PACK, sectors_all * PACK), bf16),
            dma((1,)), dma((CHUNKS,)),
            dma((1,)), dma((slots * cols,)), dma((slots * cols,)),
            dma((2,)), dma((slots * cols, 2)),
            dma((cols,)), dma((2, slots, tiles)),
            dma((2, share)), dma((2, slots, cols)),
            dma((2,)),
        ],
        compiler_params=pltpu.CompilerParams(
            collective_id=0, has_side_effects=True, vmem_limit_bytes=60000 * 1024),
    )(harmonic_table, psi_sectors, stiff_blocks, mass_blocks)
    return pl.pallas_call(
        flush, out_shape=(final, final), in_specs=[vmem, vmem], out_specs=(hbm, hbm),
        scratch_shapes=[dma((2,))], compiler_params=pltpu.CompilerParams(vmem_limit_bytes=1024 * 1024),
    )(stiff, mass)


def solution(mesh):
    placed = (P("sector", "row", None), P("row", None, None, None), P("row", None, None, None), P())
    return jax.shard_map(
        per_device,
        mesh=mesh,
        in_specs=placed,
        out_specs=(P("sector", "row", None), P("sector", "row", None)),
        check_vma=False,
    )
```

```python
import functools
import math

import jax
import jax.numpy as jnp
from jax import lax
from jax.experimental import pallas as pl
from jax.experimental.pallas import tpu as pltpu
from jax.sharding import PartitionSpec as P

MESH = pl.DeviceIdType.MESH
LANES = 128
PACK = 16
CHUNKS = 4
LEAD = 2


def flipped(index, step, count):
    total, bit = 0, 1
    while bit < count:
        total = total + bit * lax.rem(lax.div(index, bit) + (step // bit) % 2, 2)
        bit *= 2
    return total


def kernel(cfg, table_ref, psi_ref, stiff_ref, mass_ref, out_k, out_m,
           x_buf, h_buf, p_buf, pt_buf, y_buf, band, g_part, g_send, g_recv, f_send, f_row, f_col, weights,
           s1, r1, s2, r2, re, sh, rh, s3, r3, sf, rf, lb):
    n, zn, sec, rows, modes, nblk, nband, blk = cfg
    slots = sec // 2
    part = rows // n
    chunk = part // CHUNKS
    reach = nband // 2
    halo = reach * blk
    rim = halo // n
    inner = part - 2 * rim
    total = 2 * modes
    own_rows = total // zn
    halves = modes // LANES
    cols = total // LANES
    groups = slots * cols
    turn = [cols - 1 - c // 2 if c % 2 else c // 2 for c in range(cols)]
    share = zn // cols
    half = zn // 2
    tri = [c * (c + 1) // 2 for c in range(cols)]
    wide = 2 * LANES
    sectors_all = n * sec
    d = lax.axis_index("sector")
    z = lax.axis_index("row")
    order = [j for j in (2, 4, 6, 3, 5, 7) if j < n] + [1]
    order += [j for j in range(1, n) if j not in order]

    barrier = pltpu.get_barrier_semaphore()
    for j in order:
        pl.semaphore_signal(barrier, inc=1, device_id={"sector": flipped(d, j, n)}, device_id_type=MESH)
    for j in range(1, zn):
        pl.semaphore_signal(barrier, inc=1, device_id={"row": lax.rem(z + j, zn)}, device_id_type=MESH)
    pl.semaphore_wait(barrier, n - 1 + zn - 1)

    def settle(ref, sem, what):
        getattr(pltpu.make_async_remote_copy(
            src_ref=ref, dst_ref=ref, send_sem=sem, recv_sem=sem,
            device_id={"row": z}, device_id_type=MESH), what)()

    def rim_low(device):
        return pl.multiple_of(device * rim, rim)

    def rim_high(device):
        return pl.multiple_of(rows - halo + device * rim, rim)

    def middle(device, q):
        return pl.multiple_of(halo + device * inner + (q - 1) * chunk, chunk)

    def first_parts(device, q):
        if isinstance(q, int) and q == 0:
            return [(rim_low(device), 0, rim), (rim_high(device), rim, rim)]
        return [(middle(device, q), 0, chunk)]

    def first(q, j):
        target = flipped(d, j, n)
        return [pltpu.make_async_remote_copy(
            src_ref=psi_ref.at[:, pl.ds(start, count), :],
            dst_ref=x_buf.at[q, pl.ds(d * sec, sec), pl.ds(at, count), :],
            send_sem=s1.at[0], recv_sem=r1.at[q],
            device_id={"sector": target}, device_id_type=MESH) for start, at, count in first_parts(target, q)]

    def first_own(q):
        return [pltpu.make_async_copy(
            psi_ref.at[:, pl.ds(start, count), :],
            x_buf.at[q, pl.ds(d * sec, sec), pl.ds(at, count), :], r1.at[q])
            for start, at, count in first_parts(d, q)]

    partner = flipped(d, 1, n)

    def towards(core):
        return [2 * lax.div(flipped(d, j, n), 2) + core for j in order if j % 2 == 0]

    def rims(g, target):
        for start, at in ((rim_low(d), 0), (rim_high(d), rim)):
            pltpu.make_async_remote_copy(
                src_ref=h_buf.at[g, target, pl.ds(at, rim), :],
                dst_ref=p_buf.at[g, pl.ds(halo + start, rim), :],
                send_sem=s2.at[0], recv_sem=re.at[g],
                device_id={"sector": target}, device_id_type=MESH).start()

    def second(g, target, q=None):
        at, count = (2 * rim, inner) if q is None else (pl.multiple_of(2 * rim + (q - 1) * chunk, chunk), chunk)
        pltpu.make_async_remote_copy(
            src_ref=h_buf.at[g, target, pl.ds(at, count), :],
            dst_ref=p_buf.at[g, pl.ds(halo + middle(d, 1 if q is None else q), count), :],
            send_sem=s2.at[0], recv_sem=r2.at[g],
            device_id={"sector": target}, device_id_type=MESH).start()

    def edges(g):
        settle(h_buf.at[g, pl.ds(0, n - 1), pl.ds(0, 2 * rim)], re.at[g], "wait_recv")

        @pl.when(z < zn - 1)
        def _():
            edge(g, True).start()

        @pl.when(z > 0)
        def _():
            edge(g, False).start()

    def edge(g, up):
        source = rows if up else halo
        dest = 0 if up else halo + rows
        target = lax.rem(z + (1 if up else zn - 1), zn)
        return pltpu.make_async_remote_copy(
            src_ref=p_buf.at[g, pl.ds(source, halo), :],
            dst_ref=p_buf.at[g, pl.ds(dest, halo), :],
            send_sem=sh.at[int(up)], recv_sem=rh.at[g, int(up)],
            device_id={"row": target}, device_id_type=MESH)

    def first_start(q):
        for j in order:
            for copy in first(q, j):
                copy.start()
        for copy in first_own(q):
            copy.start()

    first_start(0)
    first_start(1)

    band_copies = [pltpu.make_async_copy(stiff_ref, band.at[0], lb.at[0]),
                   pltpu.make_async_copy(mass_ref, band.at[1], lb.at[1])]
    for copy in band_copies:
        copy.start()

    @pl.when(z == 0)
    def _():
        @pl.loop(0, groups)
        def _(g):
            p_buf[g, pl.ds(0, halo), :] = jnp.zeros((halo, LANES), p_buf.dtype)

    @pl.when(z == zn - 1)
    def _():
        @pl.loop(0, groups)
        def _(g):
            p_buf[g, pl.ds(halo + rows, halo), :] = jnp.zeros((halo, LANES), p_buf.dtype)

    wide_rows, wide_cols = 2 * n * PACK, sectors_all * PACK

    def spread(shape, long):
        return ((lax.broadcasted_iota(jnp.int32, shape, long) >> 4) == lax.broadcasted_iota(
            jnp.int32, shape, 1 - long)).astype(jnp.float32).astype(jnp.bfloat16)

    spread_rows = spread((wide_rows, LANES), 0)
    spread_cols = spread((LANES, wide_cols), 1)
    same = ((lax.broadcasted_iota(jnp.int32, (wide_rows, wide_cols), 0) & (PACK - 1))
            == (lax.broadcasted_iota(jnp.int32, (wide_rows, wide_cols), 1) & (PACK - 1)))
    line = lax.broadcasted_iota(jnp.int32, (LANES, LANES), 0)
    sector = lax.broadcasted_iota(jnp.int32, (LANES, LANES), 1)
    for h in range(slots):
        pair = jnp.zeros((LANES, LANES), jnp.int32)
        for e in range(n):
            pair = jnp.where((line == e) | (line == n + e), table_ref[e * slots + h], pair)
        lone = pair == 0
        upper = line >= n
        turns = jnp.where(lone & upper, sectors_all // 2, pair) * sector
        turns = turns + jnp.where(upper & jnp.logical_not(lone), sectors_all - sectors_all // 4, 0)
        turns = turns & (sectors_all - 1)
        scale = jnp.where(lone, math.sqrt(1.0 / sectors_all), math.sqrt(2.0 / sectors_all))
        value = scale * jnp.cos(turns.astype(jnp.float32) * (2.0 * math.pi / sectors_all))
        high = value.astype(jnp.bfloat16)
        low = (value - high.astype(jnp.float32)).astype(jnp.bfloat16)
        for index, piece in enumerate((high, low)):
            tall = jnp.dot(spread_rows, piece, preferred_element_type=jnp.float32).astype(jnp.bfloat16)
            full = jnp.dot(tall, spread_cols, preferred_element_type=jnp.float32)
            weights[h, index] = jnp.where(same, full, 0.0).astype(jnp.bfloat16)

    def transform(q):
        settle(x_buf.at[q], r1.at[q], "wait_recv")

        @pl.loop(0, chunk // PACK)
        def _(t):
            x = x_buf[q, :, pl.ds(pl.multiple_of(t * PACK, PACK), PACK), :].reshape(wide_cols, modes)
            at = pl.ds(pl.multiple_of(q * chunk + t * PACK, PACK), PACK)
            for h in range(slots):
                value = (jnp.dot(weights[h, 0], x, preferred_element_type=jnp.float32)
                         + jnp.dot(weights[h, 1], x, preferred_element_type=jnp.float32)).astype(jnp.bfloat16)
                for c in range(cols):
                    k, half = turn[c] // halves, turn[c] % halves
                    h_buf[h * cols + c, :, at, :] = value[
                        k * n * PACK:(k + 1) * n * PACK, half * LANES:(half + 1) * LANES].reshape(n, PACK, LANES)

    everyone = towards(0) + towards(1) + [partner]
    transform(0)
    for g in range(LEAD):
        for target in everyone:
            rims(g, target)

    @pl.loop(2, CHUNKS)
    def _(q):
        first_start(q)

    @pl.loop(0, groups)
    def _(g):
        p_buf[g, pl.ds(halo + rim_low(d), rim), :] = h_buf[g, d, pl.ds(0, rim)]
        p_buf[g, pl.ds(halo + rim_high(d), rim), :] = h_buf[g, d, pl.ds(rim, rim)]

    def middle_chunk(q):
        transform(q)
        for target in everyone:
            second(0, target, q)

    middle_chunk(1)
    for g in range(LEAD):
        edges(g)

    @pl.loop(2, CHUNKS)
    def _(q):
        middle_chunk(q)

    for target in everyone:
        rims(LEAD, target)

    @pl.loop(1, groups)
    def _(g):
        for targets in ([partner], towards(0), towards(1)):
            for target in targets:
                second(g, target)

            @pl.when(g + LEAD < groups)
            def _():
                for target in targets:
                    rims(g + LEAD, target)

    @pl.loop(0, groups)
    def _(g):
        p_buf[g, pl.ds(halo + middle(d, 1), inner), :] = h_buf[g, d, pl.ds(2 * rim, inner)]

    for copy in band_copies:
        copy.wait()

    def block_row(g, c, i):
        at = pl.ds(pl.multiple_of(i * blk, blk), blk)
        blocks = jnp.concatenate(
            [jnp.concatenate([band[which, i, k] for k in range(nband)], axis=1) for which in range(2)], axis=0)
        window = p_buf[g, pl.ds(pl.multiple_of(i * blk, blk), nband * blk), :]
        image = jnp.dot(blocks, window, preferred_element_type=jnp.float32).astype(jnp.bfloat16)
        y_buf[at, :LANES] = image[:blk]
        y_buf[at, LANES:] = image[blk:]
        pt_buf[c * LANES:(c + 1) * LANES, at] = window[halo:halo + blk].T

    def gram(h, c):
        value = jnp.dot(pt_buf[:(c + 1) * LANES, :], y_buf[...], preferred_element_type=jnp.float32)
        for b in range(c + 1):
            g_part[h, tri[c] + b] = value[b * LANES:(b + 1) * LANES]

    def owners(b, c):
        found = [(turn[b] * share + i, i, False) for i in range(share)]
        if b < c:
            found += [(turn[c] * share + i, i, True) for i in range(share)]
        return found

    def on_side(b, c, side):
        return [owner for owner in owners(b, c) if (owner[0] < half) == (side == 0)]

    def partial(h, tile, to, kind):
        return pltpu.make_async_remote_copy(
            src_ref=g_send.at[h, tile], dst_ref=g_recv.at[kind, h, tile],
            send_sem=s3.at[kind], recv_sem=r3.at[kind, h, tile],
            device_id={"row": to}, device_id_type=MESH)

    def received(h, tile, kind):
        settle(g_recv.at[kind, h, tile], r3.at[kind, h, tile], "wait_recv")
        return g_recv[kind, h, tile].astype(jnp.float32)

    def inward(h, c, p):
        for at, to in ((p, p + 1), (zn - 1 - p, zn - 2 - p)):
            @pl.when(z == at)
            def _():
                @pl.loop(0, c + 1)
                def _(b):
                    value = g_part[h, tri[c] + b]
                    if p > 0:
                        value = value + received(h, tri[c] + b, 0)
                    g_send[h, tri[c] + b] = value.astype(jnp.bfloat16)
                    partial(h, tri[c] + b, to, 0).start()

    def swap_tile(h, b, c, side):
        tile = tri[c] + b
        value = g_part[h, tile] + received(h, tile, 0)
        g_part[h, tile] = value
        if on_side(b, c, 1 - side):
            g_send[h, tile] = value.astype(jnp.bfloat16)
            partial(h, tile, half - side, 1).start()

    def final_copy(h, b, c, i, across, to):
        tile = tri[c] + b
        src = f_send.at[h, tile] if across else f_send.at[h, tile, pl.ds(i * own_rows, own_rows)]
        return pltpu.make_async_remote_copy(
            src_ref=src, dst_ref=f_col.at[h, b] if across else f_row.at[h, c],
            send_sem=sf.at[int(across)], recv_sem=rf.at[int(across), h, b if across else c],
            device_id={"row": to}, device_id_type=MESH)

    def close_tile(h, b, c, side):
        mine = on_side(b, c, side)
        if not mine:
            return
        here = half - 1 + side
        tile = tri[c] + b
        value = g_part[h, tile] + received(h, tile, 1)
        if any(to != here for to, _, _ in mine):
            f_send[h, tile] = value.astype(jnp.bfloat16)
        for to, i, across in mine:
            if to != here:
                final_copy(h, b, c, i, across, to).start()
        for to, i, across in mine:
            if to == here and across:
                keep_across(h, b, value, i)
            elif to == here:
                keep_rows(h, c, value[i * own_rows:(i + 1) * own_rows])

    def in_middle(steps):
        for side in range(2):
            @pl.when(z == half - 1 + side)
            def _():
                for step, h, b, c in steps:
                    step(h, b, c, side)

    def keep_rows(h, c, value):
        span = slice(turn[c] * LANES, (turn[c] + 1) * LANES)
        out_k[h, :, span] = value[:, :LANES]
        out_m[h, :, span] = value[:, LANES:]

    def keep_across(h, b, value, i):
        span = slice(turn[b] * LANES, (turn[b] + 1) * LANES)
        own = slice(i * own_rows, (i + 1) * own_rows)
        out_k[h, :, span] = value[:, :LANES].T[own]
        out_m[h, :, span] = value[:, LANES:].T[own]

    def older_step(h, c, p):
        if p < half - 1:
            inward(h, c, p)
        else:
            step = swap_tile if p == half - 1 else close_tile
            in_middle([(step, h, b, c) for b in range(c + 1)])

    @pl.loop(0, slots)
    def _(h):
        for c in range(cols):
            g = h * cols + c
            settle(h_buf.at[g, pl.ds(0, n - 1), pl.ds(0, inner)], r2.at[g], "wait_recv")

            @pl.when((g + 1 >= LEAD) & (g + 1 < groups))
            def _():
                edges(g + 1)

            @pl.when(z > 0)
            def _():
                edge(g, True).wait_recv()

            @pl.when(z < zn - 1)
            def _():
                edge(g, False).wait_recv()

            @pl.loop(0, nblk, unroll=4)
            def _(i):
                block_row(g, c, i)

            gram(h, c)
            inward(h, c, 0)

            for p in range(1, half + 1):
                older = (c - p) // cols
                if older == 0:
                    older_step(h, (c - p) % cols, p)
                else:
                    @pl.when(h + older >= 0)
                    def _():
                        older_step(h + older, (c - p) % cols, p)

    for t in range(1, half - 1):
        for p in range(half, t - 1, -1):
            late = groups - 1 + t - p
            older_step(late // cols, late % cols, p)
    last, end = slots - 1, cols - 1
    swaps = [(swap_tile, last, b, end) for b in range(cols)]
    before = [(close_tile, last, b, end - 1) for b in range(end)]
    closes = [(close_tile, last, b, end) for b in range(cols)]
    in_middle(swaps[:2] + before + swaps[2:3] + closes[:1] + swaps[3:] + closes[1:])

    for c in range(cols):
        for b in range(c + 1):
            for to, i, across in owners(b, c):
                if to not in (half - 1, half):
                    @pl.when(z == to)
                    def _():
                        for h in range(slots):
                            if across:
                                settle(f_col.at[h, b], rf.at[1, h, b], "wait_recv")
                                keep_across(h, b, f_col[h, b].astype(jnp.float32), i)
                            else:
                                settle(f_row.at[h, c], rf.at[0, h, c], "wait_recv")
                                keep_rows(h, c, f_row[h, c].astype(jnp.float32))

    settle(psi_ref.at[:, pl.ds(0, (n - 1) * part), :], s1.at[0], "wait_send")
    settle(h_buf.at[:, pl.ds(0, n - 1)], s2.at[0], "wait_send")

    @pl.when(z < zn - 1)
    def _():
        settle(p_buf.at[:, pl.ds(0, halo), :], sh.at[1], "wait_send")

    @pl.when(z > 0)
    def _():
        settle(p_buf.at[:, pl.ds(0, halo), :], sh.at[0], "wait_send")

    @pl.when((z != half - 1) & (z != half))
    def _():
        settle(g_send, s3.at[0], "wait_send")

    pairs = [(b, c) for c in range(cols) for b in range(c + 1)]
    for side in range(2):
        here = half - 1 + side
        sent = sum(1 for b, c in pairs if on_side(b, c, 1 - side))
        away = [owner for b, c in pairs for owner in on_side(b, c, side) if owner[0] != here]
        straight = sum(1 for owner in away if not owner[2])
        crossed = len(away) - straight

        @pl.when(z == here)
        def _():
            settle(g_send.at[:, pl.ds(0, sent)], s3.at[1], "wait_send")
            if straight:
                settle(f_send.at[:, pl.ds(0, straight), pl.ds(0, own_rows)], sf.at[0], "wait_send")
            if crossed:
                settle(f_send.at[:, pl.ds(0, crossed)], sf.at[1], "wait_send")


def flush(a_ref, b_ref, a_out, b_out, sem):
    copies = [pltpu.make_async_copy(a_ref, a_out, sem.at[0]), pltpu.make_async_copy(b_ref, b_out, sem.at[1])]
    for copy in copies:
        copy.start()
    for copy in copies:
        copy.wait()


def per_device(psi_sectors, stiff_blocks, mass_blocks, harmonic_table):
    sec, rows, modes = psi_sectors.shape
    nblk, nband, blk, _ = stiff_blocks.shape
    n, zn = lax.axis_size("sector"), lax.axis_size("row")
    sectors_all = sec * n
    slots = sec // 2
    part = rows // n
    chunk = part // CHUNKS
    halo = (nband // 2) * blk
    total = 2 * modes
    cols = total // LANES
    own_rows = total // zn
    bf16, f32 = jnp.bfloat16, jnp.float32
    dma = pltpu.SemaphoreType.DMA
    vmem = pl.BlockSpec(memory_space=pltpu.VMEM)
    hbm = pl.BlockSpec(memory_space=pl.ANY)
    tiles = cols * (cols + 1) // 2
    wide = 2 * LANES
    held = pltpu.VMEM((slots, own_rows, total), f32)
    final = jax.ShapeDtypeStruct((slots, own_rows, total), f32)
    stiff, mass = pl.pallas_call(
        functools.partial(kernel, (n, zn, sec, rows, modes, nblk, nband, blk)),
        out_shape=(held, held),
        in_specs=[pl.BlockSpec(memory_space=pltpu.SMEM), hbm, hbm, hbm],
        out_specs=(vmem, vmem),
        scratch_shapes=[
            pltpu.VMEM((CHUNKS, sectors_all, chunk, modes), bf16),
            pltpu.VMEM((slots * cols, n, part, LANES), bf16),
            pltpu.VMEM((slots * cols, rows + 2 * halo, LANES), bf16),
            pltpu.VMEM((total, rows), bf16),
            pltpu.VMEM((rows, wide), bf16),
            pltpu.VMEM((2, nblk, nband, blk, blk), bf16),
            pltpu.VMEM((slots, tiles, LANES, wide), f32),
            pltpu.VMEM((slots, tiles, LANES, wide), bf16),
            pltpu.VMEM((2, slots, tiles, LANES, wide), bf16),
            pltpu.VMEM((slots, tiles, LANES, wide), bf16),
            pltpu.VMEM((slots, cols, own_rows, wide), bf16),
            pltpu.VMEM((slots, cols, LANES, wide), bf16),
            pltpu.VMEM((slots, 2, 2 * n * PACK, sectors_all * PACK), bf16),
            dma((1,)), dma((CHUNKS,)),
            dma((1,)), dma((slots * cols,)), dma((slots * cols,)),
            dma((2,)), dma((slots * cols, 2)),
            dma((2,)), dma((2, slots, tiles)),
            dma((2,)), dma((2, slots, cols)),
            dma((2,)),
        ],
        compiler_params=pltpu.CompilerParams(
            collective_id=0, has_side_effects=True, vmem_limit_bytes=60000 * 1024),
    )(harmonic_table, psi_sectors, stiff_blocks, mass_blocks)
    return pl.pallas_call(
        flush, out_shape=(final, final), in_specs=[vmem, vmem], out_specs=(hbm, hbm),
        scratch_shapes=[dma((2,))], compiler_params=pltpu.CompilerParams(vmem_limit_bytes=1024 * 1024),
    )(stiff, mass)


def solution(mesh):
    placed = (P("sector", "row", None), P("row", None, None, None), P("row", None, None, None), P())
    return jax.shard_map(
        per_device,
        mesh=mesh,
        in_specs=placed,
        out_specs=(P("sector", "row", None), P("sector", "row", None)),
        check_vma=False,
    )
```

```python
import functools
import math

import jax
import jax.numpy as jnp
from jax import lax
from jax.experimental import pallas as pl
from jax.experimental.pallas import tpu as pltpu
from jax.sharding import PartitionSpec as P

MESH = pl.DeviceIdType.MESH
LANES = 128
PACK = 16
CHUNKS = 4
LEAD = 2


def flipped(index, step, count):
    total, bit = 0, 1
    while bit < count:
        total = total + bit * lax.rem(lax.div(index, bit) + (step // bit) % 2, 2)
        bit *= 2
    return total


def kernel(cfg, table_ref, psi_ref, stiff_ref, mass_ref, out_k, out_m,
           x_buf, h_buf, p_buf, pt_buf, y_buf, band, g_part, g_send, g_recv, f_send, f_row, f_col, weights,
           s1, r1, s2, r2, re, sh, rh, s3, r3, rd, sf, rf, lb):
    n, zn, sec, rows, modes, nblk, nband, blk = cfg
    slots = sec // 2
    part = rows // n
    chunk = part // CHUNKS
    reach = nband // 2
    halo = reach * blk
    rim = halo // n
    inner = part - 2 * rim
    total = 2 * modes
    own_rows = total // zn
    halves = modes // LANES
    cols = total // LANES
    groups = slots * cols
    turn = [cols - 1 - c // 2 if c % 2 else c // 2 for c in range(cols)]
    share = zn // cols
    half = zn // 2
    tri = [c * (c + 1) // 2 for c in range(cols)]
    wide = 2 * LANES
    sectors_all = n * sec
    d = lax.axis_index("sector")
    z = lax.axis_index("row")
    order = [j for j in (2, 4, 6, 3, 5, 7) if j < n] + [1]
    order += [j for j in range(1, n) if j not in order]

    barrier = pltpu.get_barrier_semaphore()
    for j in order:
        pl.semaphore_signal(barrier, inc=1, device_id={"sector": flipped(d, j, n)}, device_id_type=MESH)
    for j in range(1, zn):
        pl.semaphore_signal(barrier, inc=1, device_id={"row": lax.rem(z + j, zn)}, device_id_type=MESH)
    pl.semaphore_wait(barrier, n - 1 + zn - 1)

    def settle(ref, sem, what):
        getattr(pltpu.make_async_remote_copy(
            src_ref=ref, dst_ref=ref, send_sem=sem, recv_sem=sem,
            device_id={"row": z}, device_id_type=MESH), what)()

    def rim_low(device):
        return pl.multiple_of(device * rim, rim)

    def rim_high(device):
        return pl.multiple_of(rows - halo + device * rim, rim)

    def middle(device, q):
        return pl.multiple_of(halo + device * inner + (q - 1) * chunk, chunk)

    def first_parts(device, q):
        if isinstance(q, int) and q == 0:
            return [(rim_low(device), 0, rim), (rim_high(device), rim, rim)]
        return [(middle(device, q), 0, chunk)]

    def first(q, j):
        target = flipped(d, j, n)
        return [pltpu.make_async_remote_copy(
            src_ref=psi_ref.at[:, pl.ds(start, count), :],
            dst_ref=x_buf.at[q, pl.ds(d * sec, sec), pl.ds(at, count), :],
            send_sem=s1.at[0], recv_sem=r1.at[q],
            device_id={"sector": target}, device_id_type=MESH) for start, at, count in first_parts(target, q)]

    def first_own(q):
        return [pltpu.make_async_copy(
            psi_ref.at[:, pl.ds(start, count), :],
            x_buf.at[q, pl.ds(d * sec, sec), pl.ds(at, count), :], r1.at[q])
            for start, at, count in first_parts(d, q)]

    partner = flipped(d, 1, n)

    def towards(core):
        return [2 * lax.div(flipped(d, j, n), 2) + core for j in order if j % 2 == 0]

    def rims(g, target):
        for start, at in ((rim_low(d), 0), (rim_high(d), rim)):
            pltpu.make_async_remote_copy(
                src_ref=h_buf.at[g, target, pl.ds(at, rim), :],
                dst_ref=p_buf.at[g, pl.ds(halo + start, rim), :],
                send_sem=s2.at[0], recv_sem=re.at[g],
                device_id={"sector": target}, device_id_type=MESH).start()

    def second(g, target, q=None):
        at, count = (2 * rim, inner) if q is None else (pl.multiple_of(2 * rim + (q - 1) * chunk, chunk), chunk)
        pltpu.make_async_remote_copy(
            src_ref=h_buf.at[g, target, pl.ds(at, count), :],
            dst_ref=p_buf.at[g, pl.ds(halo + middle(d, 1 if q is None else q), count), :],
            send_sem=s2.at[0], recv_sem=r2.at[g],
            device_id={"sector": target}, device_id_type=MESH).start()

    def edges(g):
        settle(h_buf.at[g, pl.ds(0, n - 1), pl.ds(0, 2 * rim)], re.at[g], "wait_recv")

        @pl.when(z < zn - 1)
        def _():
            edge(g, True).start()

        @pl.when(z > 0)
        def _():
            edge(g, False).start()

    def edge(g, up):
        source = rows if up else halo
        dest = 0 if up else halo + rows
        target = lax.rem(z + (1 if up else zn - 1), zn)
        return pltpu.make_async_remote_copy(
            src_ref=p_buf.at[g, pl.ds(source, halo), :],
            dst_ref=p_buf.at[g, pl.ds(dest, halo), :],
            send_sem=sh.at[int(up)], recv_sem=rh.at[g, int(up)],
            device_id={"row": target}, device_id_type=MESH)

    def first_start(q):
        for j in order:
            for copy in first(q, j):
                copy.start()
        for copy in first_own(q):
            copy.start()

    first_start(0)
    first_start(1)

    band_copies = [pltpu.make_async_copy(stiff_ref, band.at[0], lb.at[0]),
                   pltpu.make_async_copy(mass_ref, band.at[1], lb.at[1])]
    for copy in band_copies:
        copy.start()

    @pl.when(z == 0)
    def _():
        @pl.loop(0, groups)
        def _(g):
            p_buf[g, pl.ds(0, halo), :] = jnp.zeros((halo, LANES), p_buf.dtype)

    @pl.when(z == zn - 1)
    def _():
        @pl.loop(0, groups)
        def _(g):
            p_buf[g, pl.ds(halo + rows, halo), :] = jnp.zeros((halo, LANES), p_buf.dtype)

    wide_rows, wide_cols = 2 * n * PACK, sectors_all * PACK

    def spread(shape, long):
        return ((lax.broadcasted_iota(jnp.int32, shape, long) >> 4) == lax.broadcasted_iota(
            jnp.int32, shape, 1 - long)).astype(jnp.float32).astype(jnp.bfloat16)

    spread_rows = spread((wide_rows, LANES), 0)
    spread_cols = spread((LANES, wide_cols), 1)
    same = ((lax.broadcasted_iota(jnp.int32, (wide_rows, wide_cols), 0) & (PACK - 1))
            == (lax.broadcasted_iota(jnp.int32, (wide_rows, wide_cols), 1) & (PACK - 1)))
    line = lax.broadcasted_iota(jnp.int32, (LANES, LANES), 0)
    sector = lax.broadcasted_iota(jnp.int32, (LANES, LANES), 1)
    for h in range(slots):
        pair = jnp.zeros((LANES, LANES), jnp.int32)
        for e in range(n):
            pair = jnp.where((line == e) | (line == n + e), table_ref[e * slots + h], pair)
        lone = pair == 0
        upper = line >= n
        turns = jnp.where(lone & upper, sectors_all // 2, pair) * sector
        turns = turns + jnp.where(upper & jnp.logical_not(lone), sectors_all - sectors_all // 4, 0)
        turns = turns & (sectors_all - 1)
        scale = jnp.where(lone, math.sqrt(1.0 / sectors_all), math.sqrt(2.0 / sectors_all))
        value = scale * jnp.cos(turns.astype(jnp.float32) * (2.0 * math.pi / sectors_all))
        high = value.astype(jnp.bfloat16)
        low = (value - high.astype(jnp.float32)).astype(jnp.bfloat16)
        for index, piece in enumerate((high, low)):
            tall = jnp.dot(spread_rows, piece, preferred_element_type=jnp.float32).astype(jnp.bfloat16)
            full = jnp.dot(tall, spread_cols, preferred_element_type=jnp.float32)
            weights[h, index] = jnp.where(same, full, 0.0).astype(jnp.bfloat16)

    def transform(q):
        settle(x_buf.at[q], r1.at[q], "wait_recv")

        @pl.loop(0, chunk // PACK)
        def _(t):
            x = x_buf[q, :, pl.ds(pl.multiple_of(t * PACK, PACK), PACK), :].reshape(wide_cols, modes)
            at = pl.ds(pl.multiple_of(q * chunk + t * PACK, PACK), PACK)
            for h in range(slots):
                value = (jnp.dot(weights[h, 0], x, preferred_element_type=jnp.float32)
                         + jnp.dot(weights[h, 1], x, preferred_element_type=jnp.float32)).astype(jnp.bfloat16)
                for c in range(cols):
                    k, half = turn[c] // halves, turn[c] % halves
                    h_buf[h * cols + c, :, at, :] = value[
                        k * n * PACK:(k + 1) * n * PACK, half * LANES:(half + 1) * LANES].reshape(n, PACK, LANES)

    everyone = towards(0) + towards(1) + [partner]
    transform(0)
    for g in range(LEAD):
        for target in everyone:
            rims(g, target)

    @pl.loop(2, CHUNKS)
    def _(q):
        first_start(q)

    @pl.loop(0, groups)
    def _(g):
        p_buf[g, pl.ds(halo + rim_low(d), rim), :] = h_buf[g, d, pl.ds(0, rim)]
        p_buf[g, pl.ds(halo + rim_high(d), rim), :] = h_buf[g, d, pl.ds(rim, rim)]

    def middle_chunk(q):
        transform(q)
        for target in everyone:
            second(0, target, q)

    middle_chunk(1)
    for g in range(LEAD):
        edges(g)

    @pl.loop(2, CHUNKS)
    def _(q):
        middle_chunk(q)

    for target in everyone:
        rims(LEAD, target)

    @pl.loop(1, groups)
    def _(g):
        for targets in ([partner], towards(0), towards(1)):
            for target in targets:
                second(g, target)

            @pl.when(g + LEAD < groups)
            def _():
                for target in targets:
                    rims(g + LEAD, target)

    @pl.loop(0, groups)
    def _(g):
        p_buf[g, pl.ds(halo + middle(d, 1), inner), :] = h_buf[g, d, pl.ds(2 * rim, inner)]

    for copy in band_copies:
        copy.wait()

    def block_row(g, c, i):
        at = pl.ds(pl.multiple_of(i * blk, blk), blk)
        blocks = jnp.concatenate(
            [jnp.concatenate([band[which, i, k] for k in range(nband)], axis=1) for which in range(2)], axis=0)
        window = p_buf[g, pl.ds(pl.multiple_of(i * blk, blk), nband * blk), :]
        image = jnp.dot(blocks, window, preferred_element_type=jnp.float32).astype(jnp.bfloat16)
        y_buf[at, :LANES] = image[:blk]
        y_buf[at, LANES:] = image[blk:]
        pt_buf[c * LANES:(c + 1) * LANES, at] = window[halo:halo + blk].T

    def gram(h, c):
        value = jnp.dot(pt_buf[:(c + 1) * LANES, :], y_buf[...], preferred_element_type=jnp.float32)
        for b in range(c + 1):
            g_part[h, tri[c] + b] = value[b * LANES:(b + 1) * LANES]

    def owners(b, c):
        found = [(turn[b] * share + i, i, False) for i in range(share)]
        if b < c:
            found += [(turn[c] * share + i, i, True) for i in range(share)]
        return found

    def on_side(b, c, side):
        return [owner for owner in owners(b, c) if (owner[0] < half) == (side == 0)]

    straight = half == 2
    ends = ((0, 1, 2), (zn - 1, zn - 2, zn - 3))

    def lone(b, c, side):
        return b == cols - 1 and owners(b, c)[0][0] == ends[side][2]

    def has(b, c, device):
        return any(owner[0] == device for owner in owners(b, c))

    def needed(b, c, side):
        return has(b, c, ends[side][1]) or bool(on_side(b, c, 1 - side))

    def via(b, c, side):
        return has(b, c, ends[side][0]) and has(b, c, ends[side][1])

    def reached(b, c, side):
        found = [owner[0] for owner in on_side(b, c, side)]
        return [to for to in found if not (via(b, c, side) and to == ends[side][0])]

    def tiles_of(c):
        tiles_in = list(range(c + 1))
        return tiles_in[1::-1] + tiles_in[2:] if c == cols - 1 else tiles_in

    def partial(h, tile, to, kind, held=None, sent=None):
        return pltpu.make_async_remote_copy(
            src_ref=(g_send if held is None else held).at[h, tile], dst_ref=g_recv.at[kind, h, tile],
            send_sem=s3.at[kind if sent is None else sent], recv_sem=r3.at[kind, h, tile],
            device_id={"row": to}, device_id_type=MESH)

    def lone_copy(h, tile, to):
        return pltpu.make_async_remote_copy(
            src_ref=g_send.at[h, tile], dst_ref=f_col.at[h, 0],
            send_sem=s3.at[0], recv_sem=rd.at[h],
            device_id={"row": to}, device_id_type=MESH)

    def give(h, c):
        for side, (outer, mid, far) in enumerate(ends):
            @pl.when(z == outer)
            def _():
                for b in tiles_of(c):
                    if needed(b, c, side):
                        g_send[h, tri[c] + b] = g_part[h, tri[c] + b].astype(jnp.bfloat16)
                        if lone(b, c, side):
                            lone_copy(h, tri[c] + b, far).start()
                        else:
                            partial(h, tri[c] + b, mid, 0).start()

            @pl.when(z == mid)
            def _():
                for b in tiles_of(c):
                    alone = lone(b, c, side)
                    if (has(b, c, outer) and not via(b, c, side)) or alone:
                        f_send[h, tri[c] + b] = g_part[h, tri[c] + b].astype(jnp.bfloat16)
                        partial(h, tri[c] + b, far if alone else outer, int(alone), f_send, 0).start()

    def swap_straight(h, b, c, side):
        if lone(b, c, side) or not needed(b, c, side):
            return
        tile = tri[c] + b
        value = g_part[h, tile] + received(h, tile, 0)
        if has(b, c, ends[side][1]):
            g_part[h, tile] = value
        targets = reached(b, c, 1 - side)
        if targets:
            g_send[h, tile] = value.astype(jnp.bfloat16)
            for to in targets:
                partial(h, tile, to, 1).start()

    def keep_for(h, b, c, device, value):
        for to, i, across in owners(b, c):
            if to == device and across:
                keep_across(h, b, value, i)
            elif to == device:
                keep_rows(h, c, value)

    def close_straight(h, b, c, side):
        here = ends[side][1]
        if has(b, c, here):
            value = g_part[h, tri[c] + b] + received(h, tri[c] + b, 1)
            if lone(b, c, 1 - side):
                settle(f_col.at[h, 0], rd.at[h], "wait_recv")
                value = value + f_col[h, 0].astype(jnp.float32)
            if via(b, c, side):
                f_send[h, tri[c] + b] = value.astype(jnp.bfloat16)
                partial(h, tri[c] + b, ends[side][0], 1, f_send, 0).start()
            keep_for(h, b, c, here, value)

    def received(h, tile, kind):
        settle(g_recv.at[kind, h, tile], r3.at[kind, h, tile], "wait_recv")
        return g_recv[kind, h, tile].astype(jnp.float32)

    def inward(h, c, p):
        if straight:
            return give(h, c)
        for at, to in ((p, p + 1), (zn - 1 - p, zn - 2 - p)):
            @pl.when(z == at)
            def _():
                @pl.loop(0, c + 1)
                def _(b):
                    value = g_part[h, tri[c] + b]
                    if p > 0:
                        value = value + received(h, tri[c] + b, 0)
                    g_send[h, tri[c] + b] = value.astype(jnp.bfloat16)
                    partial(h, tri[c] + b, to, 0).start()

    def swap_tile(h, b, c, side):
        if straight:
            return swap_straight(h, b, c, side)
        tile = tri[c] + b
        value = g_part[h, tile] + received(h, tile, 0)
        g_part[h, tile] = value
        if on_side(b, c, 1 - side):
            g_send[h, tile] = value.astype(jnp.bfloat16)
            partial(h, tile, half - side, 1).start()

    def final_copy(h, b, c, i, across, to):
        tile = tri[c] + b
        src = f_send.at[h, tile] if across else f_send.at[h, tile, pl.ds(i * own_rows, own_rows)]
        return pltpu.make_async_remote_copy(
            src_ref=src, dst_ref=f_col.at[h, b] if across else f_row.at[h, c],
            send_sem=sf.at[int(across)], recv_sem=rf.at[int(across), h, b if across else c],
            device_id={"row": to}, device_id_type=MESH)

    def close_tile(h, b, c, side):
        if straight:
            return close_straight(h, b, c, side)
        mine = on_side(b, c, side)
        if not mine:
            return
        here = half - 1 + side
        tile = tri[c] + b
        value = g_part[h, tile] + received(h, tile, 1)
        if any(to != here for to, _, _ in mine):
            f_send[h, tile] = value.astype(jnp.bfloat16)
        for to, i, across in mine:
            if to != here:
                final_copy(h, b, c, i, across, to).start()
        for to, i, across in mine:
            if to == here and across:
                keep_across(h, b, value, i)
            elif to == here:
                keep_rows(h, c, value[i * own_rows:(i + 1) * own_rows])

    def in_middle(steps):
        for side in range(2):
            @pl.when(z == half - 1 + side)
            def _():
                for step, h, b, c in steps:
                    step(h, b, c, side)

    def keep_rows(h, c, value):
        span = slice(turn[c] * LANES, (turn[c] + 1) * LANES)
        out_k[h, :, span] = value[:, :LANES]
        out_m[h, :, span] = value[:, LANES:]

    def keep_across(h, b, value, i):
        span = slice(turn[b] * LANES, (turn[b] + 1) * LANES)
        own = slice(i * own_rows, (i + 1) * own_rows)
        out_k[h, :, span] = value[:, :LANES].T[own]
        out_m[h, :, span] = value[:, LANES:].T[own]

    def older_step(h, c, p):
        if p < half - 1:
            inward(h, c, p)
        else:
            step = swap_tile if p == half - 1 else close_tile
            in_middle([(step, h, b, c) for b in range(c + 1)])

    @pl.loop(0, slots)
    def _(h):
        for c in range(cols):
            g = h * cols + c
            settle(h_buf.at[g, pl.ds(0, n - 1), pl.ds(0, inner)], r2.at[g], "wait_recv")

            @pl.when((g + 1 >= LEAD) & (g + 1 < groups))
            def _():
                edges(g + 1)

            @pl.when(z > 0)
            def _():
                edge(g, True).wait_recv()

            @pl.when(z < zn - 1)
            def _():
                edge(g, False).wait_recv()

            @pl.loop(0, nblk, unroll=4)
            def _(i):
                block_row(g, c, i)

            gram(h, c)
            inward(h, c, 0)

            for p in range(1, half + 1):
                older = (c - p) // cols
                if older == 0:
                    older_step(h, (c - p) % cols, p)
                else:
                    @pl.when(h + older >= 0)
                    def _():
                        older_step(h + older, (c - p) % cols, p)

    for t in range(1, half - 1):
        for p in range(half, t - 1, -1):
            late = groups - 1 + t - p
            older_step(late // cols, late % cols, p)
    last, end = slots - 1, cols - 1
    swaps = [(swap_tile, last, b, end) for b in tiles_of(end)]
    before = [(close_tile, last, b, end - 1) for b in range(end)]
    closes = [(close_tile, last, b, end) for b in tiles_of(end)]
    in_middle(swaps[:2] + before[:1] + swaps[2:3] + before[1:] + closes[:1] + swaps[3:] + closes[1:])

    if straight:
        for side, (outer, mid, far) in enumerate(ends):
            @pl.when(z == outer)
            def _():
                for h in range(slots):
                    for c in range(cols):
                        for b in range(c + 1):
                            if has(b, c, outer):
                                tile = tri[c] + b
                                value = received(h, tile, 1)
                                if not via(b, c, side):
                                    value = value + g_part[h, tile] + received(h, tile, 0)
                                keep_for(h, b, c, outer, value)
    else:
        for c in range(cols):
            for b in range(c + 1):
                for to, i, across in owners(b, c):
                    if to not in (half - 1, half):
                        @pl.when(z == to)
                        def _():
                            for h in range(slots):
                                if across:
                                    settle(f_col.at[h, b], rf.at[1, h, b], "wait_recv")
                                    keep_across(h, b, f_col[h, b].astype(jnp.float32), i)
                                else:
                                    settle(f_row.at[h, c], rf.at[0, h, c], "wait_recv")
                                    keep_rows(h, c, f_row[h, c].astype(jnp.float32))

    settle(psi_ref.at[:, pl.ds(0, (n - 1) * part), :], s1.at[0], "wait_send")
    settle(h_buf.at[:, pl.ds(0, n - 1)], s2.at[0], "wait_send")

    @pl.when(z < zn - 1)
    def _():
        settle(p_buf.at[:, pl.ds(0, halo), :], sh.at[1], "wait_send")

    @pl.when(z > 0)
    def _():
        settle(p_buf.at[:, pl.ds(0, halo), :], sh.at[0], "wait_send")

    if straight:
        pairs = [(b, c) for c in range(cols) for b in range(c + 1)]
        for side, (outer, mid, far) in enumerate(ends):
            first_sent = sum(needed(b, c, side) for b, c in pairs)
            own_sent = sum(has(b, c, outer) or lone(b, c, side) for b, c in pairs)
            half_sent = sum(len(reached(b, c, 1 - side)) for b, c in pairs if not lone(b, c, side))

            @pl.when(z == outer)
            def _():
                settle(g_send.at[:, pl.ds(0, first_sent)], s3.at[0], "wait_send")

            @pl.when(z == mid)
            def _():
                settle(g_send.at[:, pl.ds(0, own_sent)], s3.at[0], "wait_send")
                settle(g_send.at[:, pl.ds(0, half_sent)], s3.at[1], "wait_send")
        return

    @pl.when((z != half - 1) & (z != half))
    def _():
        settle(g_send, s3.at[0], "wait_send")

    pairs = [(b, c) for c in range(cols) for b in range(c + 1)]
    for side in range(2):
        here = half - 1 + side
        sent = sum(1 for b, c in pairs if on_side(b, c, 1 - side))
        away = [owner for b, c in pairs for owner in on_side(b, c, side) if owner[0] != here]
        plain = sum(1 for owner in away if not owner[2])
        crossed = len(away) - plain

        @pl.when(z == here)
        def _():
            settle(g_send.at[:, pl.ds(0, sent)], s3.at[1], "wait_send")
            if plain:
                settle(f_send.at[:, pl.ds(0, plain), pl.ds(0, own_rows)], sf.at[0], "wait_send")
            if crossed:
                settle(f_send.at[:, pl.ds(0, crossed)], sf.at[1], "wait_send")


def flush(a_ref, b_ref, a_out, b_out, sem):
    copies = [pltpu.make_async_copy(a_ref, a_out, sem.at[0]), pltpu.make_async_copy(b_ref, b_out, sem.at[1])]
    for copy in copies:
        copy.start()
    for copy in copies:
        copy.wait()


def per_device(psi_sectors, stiff_blocks, mass_blocks, harmonic_table):
    sec, rows, modes = psi_sectors.shape
    nblk, nband, blk, _ = stiff_blocks.shape
    n, zn = lax.axis_size("sector"), lax.axis_size("row")
    sectors_all = sec * n
    slots = sec // 2
    part = rows // n
    chunk = part // CHUNKS
    halo = (nband // 2) * blk
    total = 2 * modes
    cols = total // LANES
    own_rows = total // zn
    bf16, f32 = jnp.bfloat16, jnp.float32
    dma = pltpu.SemaphoreType.DMA
    vmem = pl.BlockSpec(memory_space=pltpu.VMEM)
    hbm = pl.BlockSpec(memory_space=pl.ANY)
    tiles = cols * (cols + 1) // 2
    wide = 2 * LANES
    held = pltpu.VMEM((slots, own_rows, total), f32)
    final = jax.ShapeDtypeStruct((slots, own_rows, total), f32)
    stiff, mass = pl.pallas_call(
        functools.partial(kernel, (n, zn, sec, rows, modes, nblk, nband, blk)),
        out_shape=(held, held),
        in_specs=[pl.BlockSpec(memory_space=pltpu.SMEM), hbm, hbm, hbm],
        out_specs=(vmem, vmem),
        scratch_shapes=[
            pltpu.VMEM((CHUNKS, sectors_all, chunk, modes), bf16),
            pltpu.VMEM((slots * cols, n, part, LANES), bf16),
            pltpu.VMEM((slots * cols, rows + 2 * halo, LANES), bf16),
            pltpu.VMEM((total, rows), bf16),
            pltpu.VMEM((rows, wide), bf16),
            pltpu.VMEM((2, nblk, nband, blk, blk), bf16),
            pltpu.VMEM((slots, tiles, LANES, wide), f32),
            pltpu.VMEM((slots, tiles, LANES, wide), bf16),
            pltpu.VMEM((2, slots, tiles, LANES, wide), bf16),
            pltpu.VMEM((slots, tiles, LANES, wide), bf16),
            pltpu.VMEM((slots, cols, own_rows, wide), bf16),
            pltpu.VMEM((slots, cols, LANES, wide), bf16),
            pltpu.VMEM((slots, 2, 2 * n * PACK, sectors_all * PACK), bf16),
            dma((1,)), dma((CHUNKS,)),
            dma((1,)), dma((slots * cols,)), dma((slots * cols,)),
            dma((2,)), dma((slots * cols, 2)),
            dma((2,)), dma((2, slots, tiles)), dma((slots,)),
            dma((2,)), dma((2, slots, cols) if zn != 4 else (2, 1, 1)),
            dma((2,)),
        ],
        compiler_params=pltpu.CompilerParams(
            collective_id=0, has_side_effects=True, vmem_limit_bytes=60000 * 1024),
    )(harmonic_table, psi_sectors, stiff_blocks, mass_blocks)
    return pl.pallas_call(
        flush, out_shape=(final, final), in_specs=[vmem, vmem], out_specs=(hbm, hbm),
        scratch_shapes=[dma((2,))], compiler_params=pltpu.CompilerParams(vmem_limit_bytes=1024 * 1024),
    )(stiff, mass)


def solution(mesh):
    placed = (P("sector", "row", None), P("row", None, None, None), P("row", None, None, None), P())
    return jax.shard_map(
        per_device,
        mesh=mesh,
        in_specs=placed,
        out_specs=(P("sector", "row", None), P("sector", "row", None)),
        check_vma=False,
    )
```

```python
import functools
import math

import jax
import jax.numpy as jnp
from jax import lax
from jax.experimental import pallas as pl
from jax.experimental.pallas import tpu as pltpu
from jax.sharding import PartitionSpec as P

MESH = pl.DeviceIdType.MESH
LANES = 128
PACK = 16
CHUNKS = 4
LEAD = 2


def flipped(index, step, count):
    total, bit = 0, 1
    while bit < count:
        total = total + bit * lax.rem(lax.div(index, bit) + (step // bit) % 2, 2)
        bit *= 2
    return total


def kernel(cfg, table_ref, psi_ref, stiff_ref, mass_ref, out_k, out_m,
           x_buf, h_buf, p_buf, pt_buf, y_buf, band, g_part, g_send, g_recv, f_send, f_row, f_col, weights,
           s1, r1, s2, r2, re, sh, rh, s3, r3, rd, sf, rf, lb):
    n, zn, sec, rows, modes, nblk, nband, blk = cfg
    slots = sec // 2
    part = rows // n
    chunk = part // CHUNKS
    reach = nband // 2
    halo = reach * blk
    rim = halo // n
    inner = part - 2 * rim
    total = 2 * modes
    own_rows = total // zn
    halves = modes // LANES
    cols = total // LANES
    groups = slots * cols
    turn = [cols - 1 - c // 2 if c % 2 else c // 2 for c in range(cols)]
    share = zn // cols
    half = zn // 2
    tri = [c * (c + 1) // 2 for c in range(cols)]
    wide = 2 * LANES
    sectors_all = n * sec
    d = lax.axis_index("sector")
    z = lax.axis_index("row")
    order = [j for j in (2, 4, 6, 3, 5, 7) if j < n] + [1]
    order += [j for j in range(1, n) if j not in order]

    barrier = pltpu.get_barrier_semaphore()
    for j in order:
        pl.semaphore_signal(barrier, inc=1, device_id={"sector": flipped(d, j, n)}, device_id_type=MESH)
    for j in range(1, zn):
        pl.semaphore_signal(barrier, inc=1, device_id={"row": lax.rem(z + j, zn)}, device_id_type=MESH)
    pl.semaphore_wait(barrier, n - 1 + zn - 1)

    def settle(ref, sem, what):
        getattr(pltpu.make_async_remote_copy(
            src_ref=ref, dst_ref=ref, send_sem=sem, recv_sem=sem,
            device_id={"row": z}, device_id_type=MESH), what)()

    def rim_low(device):
        return pl.multiple_of(device * rim, rim)

    def rim_high(device):
        return pl.multiple_of(rows - halo + device * rim, rim)

    def middle(device, q):
        return pl.multiple_of(halo + device * inner + (q - 1) * chunk, chunk)

    def first_parts(device, q):
        if isinstance(q, int) and q == 0:
            return [(rim_low(device), 0, rim), (rim_high(device), rim, rim)]
        return [(middle(device, q), 0, chunk)]

    def first(q, j):
        target = flipped(d, j, n)
        return [pltpu.make_async_remote_copy(
            src_ref=psi_ref.at[:, pl.ds(start, count), :],
            dst_ref=x_buf.at[q, pl.ds(d * sec, sec), pl.ds(at, count), :],
            send_sem=s1.at[0], recv_sem=r1.at[q],
            device_id={"sector": target}, device_id_type=MESH) for start, at, count in first_parts(target, q)]

    def first_own(q):
        return [pltpu.make_async_copy(
            psi_ref.at[:, pl.ds(start, count), :],
            x_buf.at[q, pl.ds(d * sec, sec), pl.ds(at, count), :], r1.at[q])
            for start, at, count in first_parts(d, q)]

    partner = flipped(d, 1, n)

    def towards(core):
        return [2 * lax.div(flipped(d, j, n), 2) + core for j in order if j % 2 == 0]

    def rims(g, target):
        for start, at in ((rim_low(d), 0), (rim_high(d), rim)):
            pltpu.make_async_remote_copy(
                src_ref=h_buf.at[g, target, pl.ds(at, rim), :],
                dst_ref=p_buf.at[g, pl.ds(halo + start, rim), :],
                send_sem=s2.at[0], recv_sem=re.at[g],
                device_id={"sector": target}, device_id_type=MESH).start()

    def second(g, target, q=None):
        at, count = (2 * rim, inner) if q is None else (pl.multiple_of(2 * rim + (q - 1) * chunk, chunk), chunk)
        pltpu.make_async_remote_copy(
            src_ref=h_buf.at[g, target, pl.ds(at, count), :],
            dst_ref=p_buf.at[g, pl.ds(halo + middle(d, 1 if q is None else q), count), :],
            send_sem=s2.at[0], recv_sem=r2.at[g],
            device_id={"sector": target}, device_id_type=MESH).start()

    def edges(g):
        settle(h_buf.at[g, pl.ds(0, n - 1), pl.ds(0, 2 * rim)], re.at[g], "wait_recv")

        @pl.when(z < zn - 1)
        def _():
            edge(g, True).start()

        @pl.when(z > 0)
        def _():
            edge(g, False).start()

    def edge(g, up):
        source = rows if up else halo
        dest = 0 if up else halo + rows
        target = lax.rem(z + (1 if up else zn - 1), zn)
        return pltpu.make_async_remote_copy(
            src_ref=p_buf.at[g, pl.ds(source, halo), :],
            dst_ref=p_buf.at[g, pl.ds(dest, halo), :],
            send_sem=sh.at[int(up)], recv_sem=rh.at[g, int(up)],
            device_id={"row": target}, device_id_type=MESH)

    def first_start(q):
        for j in order:
            for copy in first(q, j):
                copy.start()
        for copy in first_own(q):
            copy.start()

    first_start(0)
    first_start(1)

    band_copies = [pltpu.make_async_copy(stiff_ref, band.at[0], lb.at[0]),
                   pltpu.make_async_copy(mass_ref, band.at[1], lb.at[1])]
    for copy in band_copies:
        copy.start()

    @pl.when(z == 0)
    def _():
        @pl.loop(0, groups)
        def _(g):
            p_buf[g, pl.ds(0, halo), :] = jnp.zeros((halo, LANES), p_buf.dtype)

    @pl.when(z == zn - 1)
    def _():
        @pl.loop(0, groups)
        def _(g):
            p_buf[g, pl.ds(halo + rows, halo), :] = jnp.zeros((halo, LANES), p_buf.dtype)

    wide_rows, wide_cols = 2 * n * PACK, sectors_all * PACK

    def spread(shape, long):
        return ((lax.broadcasted_iota(jnp.int32, shape, long) >> 4) == lax.broadcasted_iota(
            jnp.int32, shape, 1 - long)).astype(jnp.float32).astype(jnp.bfloat16)

    spread_rows = spread((wide_rows, LANES), 0)
    spread_cols = spread((LANES, wide_cols), 1)
    same = ((lax.broadcasted_iota(jnp.int32, (wide_rows, wide_cols), 0) & (PACK - 1))
            == (lax.broadcasted_iota(jnp.int32, (wide_rows, wide_cols), 1) & (PACK - 1)))
    line = lax.broadcasted_iota(jnp.int32, (LANES, LANES), 0)
    sector = lax.broadcasted_iota(jnp.int32, (LANES, LANES), 1)
    for h in range(slots):
        pair = jnp.zeros((LANES, LANES), jnp.int32)
        for e in range(n):
            pair = jnp.where((line == e) | (line == n + e), table_ref[e * slots + h], pair)
        lone = pair == 0
        upper = line >= n
        turns = jnp.where(lone & upper, sectors_all // 2, pair) * sector
        turns = turns + jnp.where(upper & jnp.logical_not(lone), sectors_all - sectors_all // 4, 0)
        turns = turns & (sectors_all - 1)
        scale = jnp.where(lone, math.sqrt(1.0 / sectors_all), math.sqrt(2.0 / sectors_all))
        value = scale * jnp.cos(turns.astype(jnp.float32) * (2.0 * math.pi / sectors_all))
        high = value.astype(jnp.bfloat16)
        low = (value - high.astype(jnp.float32)).astype(jnp.bfloat16)
        for index, piece in enumerate((high, low)):
            tall = jnp.dot(spread_rows, piece, preferred_element_type=jnp.float32).astype(jnp.bfloat16)
            full = jnp.dot(tall, spread_cols, preferred_element_type=jnp.float32)
            weights[h, index] = jnp.where(same, full, 0.0).astype(jnp.bfloat16)

    def transform(q):
        settle(x_buf.at[q], r1.at[q], "wait_recv")

        @pl.loop(0, chunk // PACK)
        def _(t):
            x = x_buf[q, :, pl.ds(pl.multiple_of(t * PACK, PACK), PACK), :].reshape(wide_cols, modes)
            at = pl.ds(pl.multiple_of(q * chunk + t * PACK, PACK), PACK)
            for h in range(slots):
                value = (jnp.dot(weights[h, 0], x, preferred_element_type=jnp.float32)
                         + jnp.dot(weights[h, 1], x, preferred_element_type=jnp.float32)).astype(jnp.bfloat16)
                for c in range(cols):
                    k, half = turn[c] // halves, turn[c] % halves
                    h_buf[h * cols + c, :, at, :] = value[
                        k * n * PACK:(k + 1) * n * PACK, half * LANES:(half + 1) * LANES].reshape(n, PACK, LANES)

    everyone = towards(0) + towards(1) + [partner]
    transform(0)
    for g in range(LEAD):
        for target in everyone:
            rims(g, target)

    @pl.loop(2, CHUNKS)
    def _(q):
        first_start(q)

    @pl.loop(0, groups)
    def _(g):
        p_buf[g, pl.ds(halo + rim_low(d), rim), :] = h_buf[g, d, pl.ds(0, rim)]
        p_buf[g, pl.ds(halo + rim_high(d), rim), :] = h_buf[g, d, pl.ds(rim, rim)]

    def middle_chunk(q):
        transform(q)
        for target in everyone:
            second(0, target, q)

    middle_chunk(1)
    for g in range(LEAD):
        edges(g)

    @pl.loop(2, CHUNKS)
    def _(q):
        middle_chunk(q)

    for target in everyone:
        rims(LEAD, target)

    def batch(g, targets):
        for target in targets:
            second(g, target)

        @pl.when(g + LEAD < groups)
        def _():
            for target in targets:
                rims(g + LEAD, target)

    batch(jnp.int32(1), [partner] + towards(0))

    @pl.loop(1, groups - 1)
    def _(g):
        batch(g + 1, [partner] + towards(0))
        batch(g, towards(1))

    batch(jnp.int32(groups - 1), towards(1))

    @pl.loop(0, groups)
    def _(g):
        p_buf[g, pl.ds(halo + middle(d, 1), inner), :] = h_buf[g, d, pl.ds(2 * rim, inner)]

    for copy in band_copies:
        copy.wait()

    def block_row(g, c, i):
        at = pl.ds(pl.multiple_of(i * blk, blk), blk)
        blocks = jnp.concatenate(
            [jnp.concatenate([band[which, i, k] for k in range(nband)], axis=1) for which in range(2)], axis=0)
        window = p_buf[g, pl.ds(pl.multiple_of(i * blk, blk), nband * blk), :]
        image = jnp.dot(blocks, window, preferred_element_type=jnp.float32).astype(jnp.bfloat16)
        y_buf[at, :LANES] = image[:blk]
        y_buf[at, LANES:] = image[blk:]
        pt_buf[c * LANES:(c + 1) * LANES, at] = window[halo:halo + blk].T

    def gram(h, c):
        value = jnp.dot(pt_buf[:(c + 1) * LANES, :], y_buf[...], preferred_element_type=jnp.float32)
        for b in range(c + 1):
            g_part[h, tri[c] + b] = value[b * LANES:(b + 1) * LANES]

    def owners(b, c):
        found = [(turn[b] * share + i, i, False) for i in range(share)]
        if b < c:
            found += [(turn[c] * share + i, i, True) for i in range(share)]
        return found

    def on_side(b, c, side):
        return [owner for owner in owners(b, c) if (owner[0] < half) == (side == 0)]

    straight = half == 2
    ends = ((0, 1, 2), (zn - 1, zn - 2, zn - 3))

    def lone(b, c, side):
        return b == cols - 1 and owners(b, c)[0][0] == ends[side][2]

    def has(b, c, device):
        return any(owner[0] == device for owner in owners(b, c))

    def needed(b, c, side):
        return has(b, c, ends[side][1]) or bool(on_side(b, c, 1 - side))

    def via(b, c, side):
        return has(b, c, ends[side][0]) and has(b, c, ends[side][1])

    def reached(b, c, side):
        found = [owner[0] for owner in on_side(b, c, side)]
        return [to for to in found if not (via(b, c, side) and to == ends[side][0])]

    def tiles_of(c, side):
        if c < cols - 1:
            return list(range(c + 1))
        return [1, 0, *range(2, cols)] if side == 0 else [0, 2, 1, *range(3, cols)]

    def partial(h, tile, to, kind, held=None, sent=None):
        return pltpu.make_async_remote_copy(
            src_ref=(g_send if held is None else held).at[h, tile], dst_ref=g_recv.at[kind, h, tile],
            send_sem=s3.at[kind if sent is None else sent], recv_sem=r3.at[kind, h, tile],
            device_id={"row": to}, device_id_type=MESH)

    def lone_copy(h, tile, to):
        return pltpu.make_async_remote_copy(
            src_ref=g_send.at[h, tile], dst_ref=f_col.at[h, 0],
            send_sem=s3.at[0], recv_sem=rd.at[h],
            device_id={"row": to}, device_id_type=MESH)

    def give(h, c):
        for side, (outer, mid, far) in enumerate(ends):
            @pl.when(z == outer)
            def _():
                for b in tiles_of(c, side):
                    if needed(b, c, side):
                        g_send[h, tri[c] + b] = g_part[h, tri[c] + b].astype(jnp.bfloat16)
                        if lone(b, c, side):
                            lone_copy(h, tri[c] + b, far).start()
                        else:
                            partial(h, tri[c] + b, mid, 0).start()

            @pl.when(z == mid)
            def _():
                for b in tiles_of(c, side):
                    alone = lone(b, c, side)
                    if (has(b, c, outer) and not via(b, c, side)) or alone:
                        f_send[h, tri[c] + b] = g_part[h, tri[c] + b].astype(jnp.bfloat16)
                        partial(h, tri[c] + b, far if alone else outer, int(alone), f_send, 0).start()

    def swap_straight(h, b, c, side):
        if lone(b, c, side) or not needed(b, c, side):
            return
        tile = tri[c] + b
        value = g_part[h, tile] + received(h, tile, 0)
        if has(b, c, ends[side][1]):
            g_part[h, tile] = value
        targets = reached(b, c, 1 - side)
        if targets:
            g_send[h, tile] = value.astype(jnp.bfloat16)
            for to in targets:
                partial(h, tile, to, 1).start()

    def keep_for(h, b, c, device, value):
        for to, i, across in owners(b, c):
            if to == device and across:
                keep_across(h, b, value, i)
            elif to == device:
                keep_rows(h, c, value)

    def close_straight(h, b, c, side):
        here = ends[side][1]
        if has(b, c, here):
            value = g_part[h, tri[c] + b] + received(h, tri[c] + b, 1)
            if lone(b, c, 1 - side):
                settle(f_col.at[h, 0], rd.at[h], "wait_recv")
                value = value + f_col[h, 0].astype(jnp.float32)
            if via(b, c, side):
                f_send[h, tri[c] + b] = value.astype(jnp.bfloat16)
                partial(h, tri[c] + b, ends[side][0], 1, f_send, 0).start()
            keep_for(h, b, c, here, value)

    def received(h, tile, kind):
        settle(g_recv.at[kind, h, tile], r3.at[kind, h, tile], "wait_recv")
        return g_recv[kind, h, tile].astype(jnp.float32)

    def inward(h, c, p):
        if straight:
            return give(h, c)
        for at, to in ((p, p + 1), (zn - 1 - p, zn - 2 - p)):
            @pl.when(z == at)
            def _():
                @pl.loop(0, c + 1)
                def _(b):
                    value = g_part[h, tri[c] + b]
                    if p > 0:
                        value = value + received(h, tri[c] + b, 0)
                    g_send[h, tri[c] + b] = value.astype(jnp.bfloat16)
                    partial(h, tri[c] + b, to, 0).start()

    def swap_tile(h, b, c, side):
        if straight:
            return swap_straight(h, b, c, side)
        tile = tri[c] + b
        value = g_part[h, tile] + received(h, tile, 0)
        g_part[h, tile] = value
        if on_side(b, c, 1 - side):
            g_send[h, tile] = value.astype(jnp.bfloat16)
            partial(h, tile, half - side, 1).start()

    def final_copy(h, b, c, i, across, to):
        tile = tri[c] + b
        src = f_send.at[h, tile] if across else f_send.at[h, tile, pl.ds(i * own_rows, own_rows)]
        return pltpu.make_async_remote_copy(
            src_ref=src, dst_ref=f_col.at[h, b] if across else f_row.at[h, c],
            send_sem=sf.at[int(across)], recv_sem=rf.at[int(across), h, b if across else c],
            device_id={"row": to}, device_id_type=MESH)

    def close_tile(h, b, c, side):
        if straight:
            return close_straight(h, b, c, side)
        mine = on_side(b, c, side)
        if not mine:
            return
        here = half - 1 + side
        tile = tri[c] + b
        value = g_part[h, tile] + received(h, tile, 1)
        if any(to != here for to, _, _ in mine):
            f_send[h, tile] = value.astype(jnp.bfloat16)
        for to, i, across in mine:
            if to != here:
                final_copy(h, b, c, i, across, to).start()
        for to, i, across in mine:
            if to == here and across:
                keep_across(h, b, value, i)
            elif to == here:
                keep_rows(h, c, value[i * own_rows:(i + 1) * own_rows])

    def in_middle(steps):
        for side in range(2):
            @pl.when(z == half - 1 + side)
            def _():
                for step, h, b, c in steps(side):
                    step(h, b, c, side)

    def keep_rows(h, c, value):
        span = slice(turn[c] * LANES, (turn[c] + 1) * LANES)
        out_k[h, :, span] = value[:, :LANES]
        out_m[h, :, span] = value[:, LANES:]

    def keep_across(h, b, value, i):
        span = slice(turn[b] * LANES, (turn[b] + 1) * LANES)
        own = slice(i * own_rows, (i + 1) * own_rows)
        out_k[h, :, span] = value[:, :LANES].T[own]
        out_m[h, :, span] = value[:, LANES:].T[own]

    def older_step(h, c, p):
        if p < half - 1:
            inward(h, c, p)
        else:
            step = swap_tile if p == half - 1 else close_tile
            in_middle(lambda side: [(step, h, b, c) for b in range(c + 1)])

    @pl.loop(0, slots)
    def _(h):
        for c in range(cols):
            g = h * cols + c
            settle(h_buf.at[g, pl.ds(0, n - 1), pl.ds(0, inner)], r2.at[g], "wait_recv")

            @pl.when((g + 1 >= LEAD) & (g + 1 < groups))
            def _():
                edges(g + 1)

            @pl.when(z > 0)
            def _():
                edge(g, True).wait_recv()

            @pl.when(z < zn - 1)
            def _():
                edge(g, False).wait_recv()

            @pl.loop(0, nblk, unroll=8)
            def _(i):
                block_row(g, c, i)

            gram(h, c)
            inward(h, c, 0)

            for p in range(1, half + 1):
                older = (c - p) // cols
                if older == 0:
                    older_step(h, (c - p) % cols, p)
                else:
                    @pl.when(h + older >= 0)
                    def _():
                        older_step(h + older, (c - p) % cols, p)

    for t in range(1, half - 1):
        for p in range(half, t - 1, -1):
            late = groups - 1 + t - p
            older_step(late // cols, late % cols, p)
    last, end = slots - 1, cols - 1

    def finish(side):
        swaps = [(swap_tile, last, b, end) for b in tiles_of(end, side)]
        before = [(close_tile, last, b, end - 1) for b in range(end)]
        closes = [(close_tile, last, b, end) for b in tiles_of(end, 0)]
        return swaps[:1] + before[:1] + swaps[1:3] + before[1:] + closes[:1] + swaps[3:] + closes[1:]

    in_middle(finish)

    if straight:
        for side, (outer, mid, far) in enumerate(ends):
            @pl.when(z == outer)
            def _():
                for h in range(slots):
                    for c in range(cols):
                        for b in range(c + 1):
                            if has(b, c, outer):
                                tile = tri[c] + b
                                value = received(h, tile, 1)
                                if not via(b, c, side):
                                    value = value + g_part[h, tile] + received(h, tile, 0)
                                keep_for(h, b, c, outer, value)
    else:
        for c in range(cols):
            for b in range(c + 1):
                for to, i, across in owners(b, c):
                    if to not in (half - 1, half):
                        @pl.when(z == to)
                        def _():
                            for h in range(slots):
                                if across:
                                    settle(f_col.at[h, b], rf.at[1, h, b], "wait_recv")
                                    keep_across(h, b, f_col[h, b].astype(jnp.float32), i)
                                else:
                                    settle(f_row.at[h, c], rf.at[0, h, c], "wait_recv")
                                    keep_rows(h, c, f_row[h, c].astype(jnp.float32))

    settle(psi_ref.at[:, pl.ds(0, (n - 1) * part), :], s1.at[0], "wait_send")
    settle(h_buf.at[:, pl.ds(0, n - 1)], s2.at[0], "wait_send")

    @pl.when(z < zn - 1)
    def _():
        settle(p_buf.at[:, pl.ds(0, halo), :], sh.at[1], "wait_send")

    @pl.when(z > 0)
    def _():
        settle(p_buf.at[:, pl.ds(0, halo), :], sh.at[0], "wait_send")

    if straight:
        pairs = [(b, c) for c in range(cols) for b in range(c + 1)]
        for side, (outer, mid, far) in enumerate(ends):
            first_sent = sum(needed(b, c, side) for b, c in pairs)
            own_sent = sum(has(b, c, outer) or lone(b, c, side) for b, c in pairs)
            half_sent = sum(len(reached(b, c, 1 - side)) for b, c in pairs if not lone(b, c, side))

            @pl.when(z == outer)
            def _():
                settle(g_send.at[:, pl.ds(0, first_sent)], s3.at[0], "wait_send")

            @pl.when(z == mid)
            def _():
                settle(g_send.at[:, pl.ds(0, own_sent)], s3.at[0], "wait_send")
                settle(g_send.at[:, pl.ds(0, half_sent)], s3.at[1], "wait_send")
        return

    @pl.when((z != half - 1) & (z != half))
    def _():
        settle(g_send, s3.at[0], "wait_send")

    pairs = [(b, c) for c in range(cols) for b in range(c + 1)]
    for side in range(2):
        here = half - 1 + side
        sent = sum(1 for b, c in pairs if on_side(b, c, 1 - side))
        away = [owner for b, c in pairs for owner in on_side(b, c, side) if owner[0] != here]
        plain = sum(1 for owner in away if not owner[2])
        crossed = len(away) - plain

        @pl.when(z == here)
        def _():
            settle(g_send.at[:, pl.ds(0, sent)], s3.at[1], "wait_send")
            if plain:
                settle(f_send.at[:, pl.ds(0, plain), pl.ds(0, own_rows)], sf.at[0], "wait_send")
            if crossed:
                settle(f_send.at[:, pl.ds(0, crossed)], sf.at[1], "wait_send")


def flush(a_ref, b_ref, a_out, b_out, sem):
    copies = [pltpu.make_async_copy(a_ref, a_out, sem.at[0]), pltpu.make_async_copy(b_ref, b_out, sem.at[1])]
    for copy in copies:
        copy.start()
    for copy in copies:
        copy.wait()


def per_device(psi_sectors, stiff_blocks, mass_blocks, harmonic_table):
    sec, rows, modes = psi_sectors.shape
    nblk, nband, blk, _ = stiff_blocks.shape
    n, zn = lax.axis_size("sector"), lax.axis_size("row")
    sectors_all = sec * n
    slots = sec // 2
    part = rows // n
    chunk = part // CHUNKS
    halo = (nband // 2) * blk
    total = 2 * modes
    cols = total // LANES
    own_rows = total // zn
    bf16, f32 = jnp.bfloat16, jnp.float32
    dma = pltpu.SemaphoreType.DMA
    vmem = pl.BlockSpec(memory_space=pltpu.VMEM)
    hbm = pl.BlockSpec(memory_space=pl.ANY)
    tiles = cols * (cols + 1) // 2
    wide = 2 * LANES
    held = pltpu.VMEM((slots, own_rows, total), f32)
    final = jax.ShapeDtypeStruct((slots, own_rows, total), f32)
    stiff, mass = pl.pallas_call(
        functools.partial(kernel, (n, zn, sec, rows, modes, nblk, nband, blk)),
        out_shape=(held, held),
        in_specs=[pl.BlockSpec(memory_space=pltpu.SMEM), hbm, hbm, hbm],
        out_specs=(vmem, vmem),
        scratch_shapes=[
            pltpu.VMEM((CHUNKS, sectors_all, chunk, modes), bf16),
            pltpu.VMEM((slots * cols, n, part, LANES), bf16),
            pltpu.VMEM((slots * cols, rows + 2 * halo, LANES), bf16),
            pltpu.VMEM((total, rows), bf16),
            pltpu.VMEM((rows, wide), bf16),
            pltpu.VMEM((2, nblk, nband, blk, blk), bf16),
            pltpu.VMEM((slots, tiles, LANES, wide), f32),
            pltpu.VMEM((slots, tiles, LANES, wide), bf16),
            pltpu.VMEM((2, slots, tiles, LANES, wide), bf16),
            pltpu.VMEM((slots, tiles, LANES, wide), bf16),
            pltpu.VMEM((slots, cols, own_rows, wide), bf16),
            pltpu.VMEM((slots, cols, LANES, wide), bf16),
            pltpu.VMEM((slots, 2, 2 * n * PACK, sectors_all * PACK), bf16),
            dma((1,)), dma((CHUNKS,)),
            dma((1,)), dma((slots * cols,)), dma((slots * cols,)),
            dma((2,)), dma((slots * cols, 2)),
            dma((2,)), dma((2, slots, tiles)), dma((slots,)),
            dma((2,)), dma((2, slots, cols) if zn != 4 else (2, 1, 1)),
            dma((2,)),
        ],
        compiler_params=pltpu.CompilerParams(
            collective_id=0, has_side_effects=True, vmem_limit_bytes=60000 * 1024),
    )(harmonic_table, psi_sectors, stiff_blocks, mass_blocks)
    return pl.pallas_call(
        flush, out_shape=(final, final), in_specs=[vmem, vmem], out_specs=(hbm, hbm),
        scratch_shapes=[dma((2,))], compiler_params=pltpu.CompilerParams(vmem_limit_bytes=1024 * 1024),
    )(stiff, mass)


def solution(mesh):
    placed = (P("sector", "row", None), P("row", None, None, None), P("row", None, None, None), P())
    return jax.shard_map(
        per_device,
        mesh=mesh,
        in_specs=placed,
        out_specs=(P("sector", "row", None), P("sector", "row", None)),
        check_vma=False,
    )
```

```python
import functools
import math

import jax
import jax.numpy as jnp
from jax import lax
from jax.experimental import pallas as pl
from jax.experimental.pallas import tpu as pltpu
from jax.sharding import PartitionSpec as P

MESH = pl.DeviceIdType.MESH
LANES = 128
PACK = 16
CHUNKS = 4
LEAD = 2


def flipped(index, step, count):
    total, bit = 0, 1
    while bit < count:
        total = total + bit * lax.rem(lax.div(index, bit) + (step // bit) % 2, 2)
        bit *= 2
    return total


def kernel(cfg, table_ref, psi_ref, stiff_ref, mass_ref, out_k, out_m,
           x_buf, h_buf, p_buf, pt_buf, y_buf, band, g_part, g_send, g_recv, f_send, f_row, f_col, weights,
           s1, r1, s2, r2, re, sh, rh, s3, r3, rd, sf, rf, lb):
    n, zn, sec, rows, modes, nblk, nband, blk = cfg
    slots = sec // 2
    part = rows // n
    chunk = part // CHUNKS
    reach = nband // 2
    halo = reach * blk
    rim = halo // n
    inner = part - 2 * rim
    total = 2 * modes
    own_rows = total // zn
    halves = modes // LANES
    cols = total // LANES
    groups = slots * cols
    turn = [cols - 1 - c // 2 if c % 2 else c // 2 for c in range(cols)]
    share = zn // cols
    half = zn // 2
    tri = [c * (c + 1) // 2 for c in range(cols)]
    wide = 2 * LANES
    sectors_all = n * sec
    d = lax.axis_index("sector")
    z = lax.axis_index("row")
    order = [j for j in (6, 2, 4, 7, 3, 5) if j < n] + [1]
    order += [j for j in range(1, n) if j not in order]

    barrier = pltpu.get_barrier_semaphore()
    for j in order:
        pl.semaphore_signal(barrier, inc=1, device_id={"sector": flipped(d, j, n)}, device_id_type=MESH)
    for j in range(1, zn):
        pl.semaphore_signal(barrier, inc=1, device_id={"row": lax.rem(z + j, zn)}, device_id_type=MESH)
    pl.semaphore_wait(barrier, n - 1 + zn - 1)

    def settle(ref, sem, what):
        getattr(pltpu.make_async_remote_copy(
            src_ref=ref, dst_ref=ref, send_sem=sem, recv_sem=sem,
            device_id={"row": z}, device_id_type=MESH), what)()

    def rim_low(device):
        return pl.multiple_of(device * rim, rim)

    def rim_high(device):
        return pl.multiple_of(rows - halo + device * rim, rim)

    def middle(device, q):
        return pl.multiple_of(halo + device * inner + (q - 1) * chunk, chunk)

    def first_parts(device, q):
        if isinstance(q, int) and q == 0:
            return [(rim_low(device), 0, rim), (rim_high(device), rim, rim)]
        return [(middle(device, q), 0, chunk)]

    def first(q, j):
        target = flipped(d, j, n)
        return [pltpu.make_async_remote_copy(
            src_ref=psi_ref.at[:, pl.ds(start, count), :],
            dst_ref=x_buf.at[q, pl.ds(d * sec, sec), pl.ds(at, count), :],
            send_sem=s1.at[0], recv_sem=r1.at[q],
            device_id={"sector": target}, device_id_type=MESH) for start, at, count in first_parts(target, q)]

    def first_own(q):
        return [pltpu.make_async_copy(
            psi_ref.at[:, pl.ds(start, count), :],
            x_buf.at[q, pl.ds(d * sec, sec), pl.ds(at, count), :], r1.at[q])
            for start, at, count in first_parts(d, q)]

    partner = flipped(d, 1, n)

    def towards(core):
        return [2 * lax.div(flipped(d, j, n), 2) + core for j in order if j % 2 == 0]

    def rims(g, target):
        for start, at in ((rim_low(d), 0), (rim_high(d), rim)):
            pltpu.make_async_remote_copy(
                src_ref=h_buf.at[g, target, pl.ds(at, rim), :],
                dst_ref=p_buf.at[g, pl.ds(halo + start, rim), :],
                send_sem=s2.at[0], recv_sem=re.at[g],
                device_id={"sector": target}, device_id_type=MESH).start()

    def second(g, target, q=None):
        at, count = (2 * rim, inner) if q is None else (pl.multiple_of(2 * rim + (q - 1) * chunk, chunk), chunk)
        pltpu.make_async_remote_copy(
            src_ref=h_buf.at[g, target, pl.ds(at, count), :],
            dst_ref=p_buf.at[g, pl.ds(halo + middle(d, 1 if q is None else q), count), :],
            send_sem=s2.at[0], recv_sem=r2.at[g],
            device_id={"sector": target}, device_id_type=MESH).start()

    def edges(g):
        settle(h_buf.at[g, pl.ds(0, n - 1), pl.ds(0, 2 * rim)], re.at[g], "wait_recv")

        @pl.when(z < zn - 1)
        def _():
            edge(g, True).start()

        @pl.when(z > 0)
        def _():
            edge(g, False).start()

    def edge(g, up):
        source = rows if up else halo
        dest = 0 if up else halo + rows
        target = lax.rem(z + (1 if up else zn - 1), zn)
        return pltpu.make_async_remote_copy(
            src_ref=p_buf.at[g, pl.ds(source, halo), :],
            dst_ref=p_buf.at[g, pl.ds(dest, halo), :],
            send_sem=sh.at[int(up)], recv_sem=rh.at[g, int(up)],
            device_id={"row": target}, device_id_type=MESH)

    def first_start(q):
        for j in order:
            for copy in first(q, j):
                copy.start()
        for copy in first_own(q):
            copy.start()

    first_start(0)
    first_start(1)

    band_copies = [pltpu.make_async_copy(stiff_ref, band.at[0], lb.at[0]),
                   pltpu.make_async_copy(mass_ref, band.at[1], lb.at[1])]
    for copy in band_copies:
        copy.start()

    @pl.when(z == 0)
    def _():
        @pl.loop(0, groups)
        def _(g):
            p_buf[g, pl.ds(0, halo), :] = jnp.zeros((halo, LANES), p_buf.dtype)

    @pl.when(z == zn - 1)
    def _():
        @pl.loop(0, groups)
        def _(g):
            p_buf[g, pl.ds(halo + rows, halo), :] = jnp.zeros((halo, LANES), p_buf.dtype)

    wide_rows, wide_cols = 2 * n * PACK, sectors_all * PACK

    def spread(shape, long):
        return ((lax.broadcasted_iota(jnp.int32, shape, long) >> 4) == lax.broadcasted_iota(
            jnp.int32, shape, 1 - long)).astype(jnp.float32).astype(jnp.bfloat16)

    spread_rows = spread((wide_rows, LANES), 0)
    spread_cols = spread((LANES, wide_cols), 1)
    same = ((lax.broadcasted_iota(jnp.int32, (wide_rows, wide_cols), 0) & (PACK - 1))
            == (lax.broadcasted_iota(jnp.int32, (wide_rows, wide_cols), 1) & (PACK - 1)))
    line = lax.broadcasted_iota(jnp.int32, (LANES, LANES), 0)
    sector = lax.broadcasted_iota(jnp.int32, (LANES, LANES), 1)
    for h in range(slots):
        pair = jnp.zeros((LANES, LANES), jnp.int32)
        for e in range(n):
            pair = jnp.where((line == e) | (line == n + e), table_ref[e * slots + h], pair)
        lone = pair == 0
        upper = line >= n
        turns = jnp.where(lone & upper, sectors_all // 2, pair) * sector
        turns = turns + jnp.where(upper & jnp.logical_not(lone), sectors_all - sectors_all // 4, 0)
        turns = turns & (sectors_all - 1)
        scale = jnp.where(lone, math.sqrt(1.0 / sectors_all), math.sqrt(2.0 / sectors_all))
        value = scale * jnp.cos(turns.astype(jnp.float32) * (2.0 * math.pi / sectors_all))
        high = value.astype(jnp.bfloat16)
        low = (value - high.astype(jnp.float32)).astype(jnp.bfloat16)
        for index, piece in enumerate((high, low)):
            tall = jnp.dot(spread_rows, piece, preferred_element_type=jnp.float32).astype(jnp.bfloat16)
            full = jnp.dot(tall, spread_cols, preferred_element_type=jnp.float32)
            weights[h, index] = jnp.where(same, full, 0.0).astype(jnp.bfloat16)

    def transform(q):
        settle(x_buf.at[q], r1.at[q], "wait_recv")

        @pl.loop(0, chunk // PACK)
        def _(t):
            x = x_buf[q, :, pl.ds(pl.multiple_of(t * PACK, PACK), PACK), :].reshape(wide_cols, modes)
            at = pl.ds(pl.multiple_of(q * chunk + t * PACK, PACK), PACK)
            for h in range(slots):
                value = (jnp.dot(weights[h, 0], x, preferred_element_type=jnp.float32)
                         + jnp.dot(weights[h, 1], x, preferred_element_type=jnp.float32)).astype(jnp.bfloat16)
                for c in range(cols):
                    k, half = turn[c] // halves, turn[c] % halves
                    h_buf[h * cols + c, :, at, :] = value[
                        k * n * PACK:(k + 1) * n * PACK, half * LANES:(half + 1) * LANES].reshape(n, PACK, LANES)

    everyone = towards(0) + towards(1) + [partner]
    transform(0)
    for g in range(LEAD):
        for target in everyone:
            rims(g, target)

    @pl.loop(2, CHUNKS)
    def _(q):
        first_start(q)

    @pl.loop(0, groups)
    def _(g):
        p_buf[g, pl.ds(halo + rim_low(d), rim), :] = h_buf[g, d, pl.ds(0, rim)]
        p_buf[g, pl.ds(halo + rim_high(d), rim), :] = h_buf[g, d, pl.ds(rim, rim)]

    def middle_chunk(q):
        transform(q)
        for target in everyone:
            second(0, target, q)

    middle_chunk(1)
    for g in range(LEAD):
        edges(g)

    @pl.loop(2, CHUNKS)
    def _(q):
        middle_chunk(q)

    for target in everyone:
        rims(LEAD, target)

    def batch(g, targets):
        for target in targets:
            second(g, target)

        @pl.when(g + LEAD < groups)
        def _():
            for target in targets:
                rims(g + LEAD, target)

    batch(jnp.int32(1), [partner] + towards(0))

    @pl.loop(1, groups - 1)
    def _(g):
        batch(g + 1, [partner] + towards(0))
        batch(g, towards(1))

    batch(jnp.int32(groups - 1), towards(1))

    @pl.loop(0, groups)
    def _(g):
        p_buf[g, pl.ds(halo + middle(d, 1), inner), :] = h_buf[g, d, pl.ds(2 * rim, inner)]

    for copy in band_copies:
        copy.wait()

    def block_row(g, c, i):
        at = pl.ds(pl.multiple_of(i * blk, blk), blk)
        blocks = jnp.concatenate(
            [jnp.concatenate([band[which, i, k] for k in range(nband)], axis=1) for which in range(2)], axis=0)
        window = p_buf[g, pl.ds(pl.multiple_of(i * blk, blk), nband * blk), :]
        image = jnp.dot(blocks, window, preferred_element_type=jnp.float32).astype(jnp.bfloat16)
        y_buf[at, :LANES] = image[:blk]
        y_buf[at, LANES:] = image[blk:]
        pt_buf[c * LANES:(c + 1) * LANES, at] = window[halo:halo + blk].T

    def gram(h, c):
        value = jnp.dot(pt_buf[:(c + 1) * LANES, :], y_buf[...], preferred_element_type=jnp.float32)
        for b in range(c + 1):
            g_part[h, tri[c] + b] = value[b * LANES:(b + 1) * LANES]

    def owners(b, c):
        found = [(turn[b] * share + i, i, False) for i in range(share)]
        if b < c:
            found += [(turn[c] * share + i, i, True) for i in range(share)]
        return found

    def on_side(b, c, side):
        return [owner for owner in owners(b, c) if (owner[0] < half) == (side == 0)]

    straight = half == 2
    ends = ((0, 1, 2), (zn - 1, zn - 2, zn - 3))

    def lone(b, c, side):
        return b == cols - 1 and owners(b, c)[0][0] == ends[side][2]

    def has(b, c, device):
        return any(owner[0] == device for owner in owners(b, c))

    def needed(b, c, side):
        return has(b, c, ends[side][1]) or bool(on_side(b, c, 1 - side))

    def via(b, c, side):
        return has(b, c, ends[side][0]) and has(b, c, ends[side][1])

    def reached(b, c, side):
        found = [owner[0] for owner in on_side(b, c, side)]
        return [to for to in found if not (via(b, c, side) and to == ends[side][0])]

    def tiles_of(c, side):
        if c < cols - 1:
            return list(range(c + 1))
        return [1, 0, *range(2, cols)] if side == 0 else [0, 2, 1, *range(3, cols)]

    def partial(h, tile, to, kind, held=None, sent=None):
        return pltpu.make_async_remote_copy(
            src_ref=(g_send if held is None else held).at[h, tile], dst_ref=g_recv.at[kind, h, tile],
            send_sem=s3.at[kind if sent is None else sent], recv_sem=r3.at[kind, h, tile],
            device_id={"row": to}, device_id_type=MESH)

    def lone_copy(h, tile, to):
        return pltpu.make_async_remote_copy(
            src_ref=g_send.at[h, tile], dst_ref=f_col.at[h, 0],
            send_sem=s3.at[0], recv_sem=rd.at[h],
            device_id={"row": to}, device_id_type=MESH)

    def give(h, c):
        for side, (outer, mid, far) in enumerate(ends):
            @pl.when(z == outer)
            def _():
                for b in tiles_of(c, side):
                    if needed(b, c, side):
                        g_send[h, tri[c] + b] = g_part[h, tri[c] + b].astype(jnp.bfloat16)
                        if lone(b, c, side):
                            lone_copy(h, tri[c] + b, far).start()
                        else:
                            partial(h, tri[c] + b, mid, 0).start()

            @pl.when(z == mid)
            def _():
                for b in tiles_of(c, side):
                    alone = lone(b, c, side)
                    if (has(b, c, outer) and not via(b, c, side)) or alone:
                        f_send[h, tri[c] + b] = g_part[h, tri[c] + b].astype(jnp.bfloat16)
                        partial(h, tri[c] + b, far if alone else outer, int(alone), f_send, 0).start()

    def swap_straight(h, b, c, side):
        if lone(b, c, side) or not needed(b, c, side):
            return
        tile = tri[c] + b
        value = g_part[h, tile] + received(h, tile, 0)
        if has(b, c, ends[side][1]):
            g_part[h, tile] = value
        targets = reached(b, c, 1 - side)
        if targets:
            g_send[h, tile] = value.astype(jnp.bfloat16)
            for to in targets:
                partial(h, tile, to, 1).start()

    def keep_for(h, b, c, device, value):
        for to, i, across in owners(b, c):
            if to == device and across:
                keep_across(h, b, value, i)
            elif to == device:
                keep_rows(h, c, value)

    def close_straight(h, b, c, side):
        here = ends[side][1]
        if has(b, c, here):
            value = g_part[h, tri[c] + b] + received(h, tri[c] + b, 1)
            if lone(b, c, 1 - side):
                settle(f_col.at[h, 0], rd.at[h], "wait_recv")
                value = value + f_col[h, 0].astype(jnp.float32)
            if via(b, c, side):
                f_send[h, tri[c] + b] = value.astype(jnp.bfloat16)
                partial(h, tri[c] + b, ends[side][0], 1, f_send, 0).start()
            keep_for(h, b, c, here, value)

    def received(h, tile, kind):
        settle(g_recv.at[kind, h, tile], r3.at[kind, h, tile], "wait_recv")
        return g_recv[kind, h, tile].astype(jnp.float32)

    def inward(h, c, p):
        if straight:
            return give(h, c)
        for at, to in ((p, p + 1), (zn - 1 - p, zn - 2 - p)):
            @pl.when(z == at)
            def _():
                @pl.loop(0, c + 1)
                def _(b):
                    value = g_part[h, tri[c] + b]
                    if p > 0:
                        value = value + received(h, tri[c] + b, 0)
                    g_send[h, tri[c] + b] = value.astype(jnp.bfloat16)
                    partial(h, tri[c] + b, to, 0).start()

    def swap_tile(h, b, c, side):
        if straight:
            return swap_straight(h, b, c, side)
        tile = tri[c] + b
        value = g_part[h, tile] + received(h, tile, 0)
        g_part[h, tile] = value
        if on_side(b, c, 1 - side):
            g_send[h, tile] = value.astype(jnp.bfloat16)
            partial(h, tile, half - side, 1).start()

    def final_copy(h, b, c, i, across, to):
        tile = tri[c] + b
        src = f_send.at[h, tile] if across else f_send.at[h, tile, pl.ds(i * own_rows, own_rows)]
        return pltpu.make_async_remote_copy(
            src_ref=src, dst_ref=f_col.at[h, b] if across else f_row.at[h, c],
            send_sem=sf.at[int(across)], recv_sem=rf.at[int(across), h, b if across else c],
            device_id={"row": to}, device_id_type=MESH)

    def close_tile(h, b, c, side):
        if straight:
            return close_straight(h, b, c, side)
        mine = on_side(b, c, side)
        if not mine:
            return
        here = half - 1 + side
        tile = tri[c] + b
        value = g_part[h, tile] + received(h, tile, 1)
        if any(to != here for to, _, _ in mine):
            f_send[h, tile] = value.astype(jnp.bfloat16)
        for to, i, across in mine:
            if to != here:
                final_copy(h, b, c, i, across, to).start()
        for to, i, across in mine:
            if to == here and across:
                keep_across(h, b, value, i)
            elif to == here:
                keep_rows(h, c, value[i * own_rows:(i + 1) * own_rows])

    def in_middle(steps):
        for side in range(2):
            @pl.when(z == half - 1 + side)
            def _():
                for step, h, b, c in steps(side):
                    step(h, b, c, side)

    def keep_rows(h, c, value):
        span = slice(turn[c] * LANES, (turn[c] + 1) * LANES)
        out_k[h, :, span] = value[:, :LANES]
        out_m[h, :, span] = value[:, LANES:]

    def keep_across(h, b, value, i):
        span = slice(turn[b] * LANES, (turn[b] + 1) * LANES)
        own = slice(i * own_rows, (i + 1) * own_rows)
        out_k[h, :, span] = value[:, :LANES].T[own]
        out_m[h, :, span] = value[:, LANES:].T[own]

    def older_step(h, c, p):
        if p < half - 1:
            inward(h, c, p)
        else:
            step = swap_tile if p == half - 1 else close_tile
            in_middle(lambda side: [(step, h, b, c) for b in range(c + 1)])

    @pl.loop(0, slots)
    def _(h):
        for c in range(cols):
            g = h * cols + c
            settle(h_buf.at[g, pl.ds(0, n - 1), pl.ds(0, inner)], r2.at[g], "wait_recv")

            @pl.when((g + 1 >= LEAD) & (g + 1 < groups))
            def _():
                edges(g + 1)

            @pl.when(z > 0)
            def _():
                edge(g, True).wait_recv()

            @pl.when(z < zn - 1)
            def _():
                edge(g, False).wait_recv()

            @pl.loop(0, nblk, unroll=8)
            def _(i):
                block_row(g, c, i)

            gram(h, c)
            inward(h, c, 0)

            for p in range(1, half + 1):
                older = (c - p) // cols
                if older == 0:
                    older_step(h, (c - p) % cols, p)
                else:
                    @pl.when(h + older >= 0)
                    def _():
                        older_step(h + older, (c - p) % cols, p)

    for t in range(1, half - 1):
        for p in range(half, t - 1, -1):
            late = groups - 1 + t - p
            older_step(late // cols, late % cols, p)
    last, end = slots - 1, cols - 1

    def finish(side):
        swaps = [(swap_tile, last, b, end) for b in tiles_of(end, side)]
        before = [(close_tile, last, b, end - 1) for b in range(end)]
        closes = [(close_tile, last, b, end) for b in tiles_of(end, 0)]
        return swaps[:1] + before[:1] + swaps[1:3] + before[1:] + closes[:1] + swaps[3:] + closes[1:]

    in_middle(finish)

    if straight:
        for side, (outer, mid, far) in enumerate(ends):
            @pl.when(z == outer)
            def _():
                for h in range(slots):
                    for c in range(cols):
                        for b in range(c + 1):
                            if has(b, c, outer):
                                tile = tri[c] + b
                                value = received(h, tile, 1)
                                if not via(b, c, side):
                                    value = value + g_part[h, tile] + received(h, tile, 0)
                                keep_for(h, b, c, outer, value)
    else:
        for c in range(cols):
            for b in range(c + 1):
                for to, i, across in owners(b, c):
                    if to not in (half - 1, half):
                        @pl.when(z == to)
                        def _():
                            for h in range(slots):
                                if across:
                                    settle(f_col.at[h, b], rf.at[1, h, b], "wait_recv")
                                    keep_across(h, b, f_col[h, b].astype(jnp.float32), i)
                                else:
                                    settle(f_row.at[h, c], rf.at[0, h, c], "wait_recv")
                                    keep_rows(h, c, f_row[h, c].astype(jnp.float32))

    settle(psi_ref.at[:, pl.ds(0, (n - 1) * part), :], s1.at[0], "wait_send")
    settle(h_buf.at[:, pl.ds(0, n - 1)], s2.at[0], "wait_send")

    @pl.when(z < zn - 1)
    def _():
        settle(p_buf.at[:, pl.ds(0, halo), :], sh.at[1], "wait_send")

    @pl.when(z > 0)
    def _():
        settle(p_buf.at[:, pl.ds(0, halo), :], sh.at[0], "wait_send")

    if straight:
        pairs = [(b, c) for c in range(cols) for b in range(c + 1)]
        for side, (outer, mid, far) in enumerate(ends):
            first_sent = sum(needed(b, c, side) for b, c in pairs)
            own_sent = sum(has(b, c, outer) or lone(b, c, side) for b, c in pairs)
            half_sent = sum(len(reached(b, c, 1 - side)) for b, c in pairs if not lone(b, c, side))

            @pl.when(z == outer)
            def _():
                settle(g_send.at[:, pl.ds(0, first_sent)], s3.at[0], "wait_send")

            @pl.when(z == mid)
            def _():
                settle(g_send.at[:, pl.ds(0, own_sent)], s3.at[0], "wait_send")
                settle(g_send.at[:, pl.ds(0, half_sent)], s3.at[1], "wait_send")
        return

    @pl.when((z != half - 1) & (z != half))
    def _():
        settle(g_send, s3.at[0], "wait_send")

    pairs = [(b, c) for c in range(cols) for b in range(c + 1)]
    for side in range(2):
        here = half - 1 + side
        sent = sum(1 for b, c in pairs if on_side(b, c, 1 - side))
        away = [owner for b, c in pairs for owner in on_side(b, c, side) if owner[0] != here]
        plain = sum(1 for owner in away if not owner[2])
        crossed = len(away) - plain

        @pl.when(z == here)
        def _():
            settle(g_send.at[:, pl.ds(0, sent)], s3.at[1], "wait_send")
            if plain:
                settle(f_send.at[:, pl.ds(0, plain), pl.ds(0, own_rows)], sf.at[0], "wait_send")
            if crossed:
                settle(f_send.at[:, pl.ds(0, crossed)], sf.at[1], "wait_send")


def flush(a_ref, b_ref, a_out, b_out, sem):
    copies = [pltpu.make_async_copy(a_ref, a_out, sem.at[0]), pltpu.make_async_copy(b_ref, b_out, sem.at[1])]
    for copy in copies:
        copy.start()
    for copy in copies:
        copy.wait()


def per_device(psi_sectors, stiff_blocks, mass_blocks, harmonic_table):
    sec, rows, modes = psi_sectors.shape
    nblk, nband, blk, _ = stiff_blocks.shape
    n, zn = lax.axis_size("sector"), lax.axis_size("row")
    sectors_all = sec * n
    slots = sec // 2
    part = rows // n
    chunk = part // CHUNKS
    halo = (nband // 2) * blk
    total = 2 * modes
    cols = total // LANES
    own_rows = total // zn
    bf16, f32 = jnp.bfloat16, jnp.float32
    dma = pltpu.SemaphoreType.DMA
    vmem = pl.BlockSpec(memory_space=pltpu.VMEM)
    hbm = pl.BlockSpec(memory_space=pl.ANY)
    tiles = cols * (cols + 1) // 2
    wide = 2 * LANES
    held = pltpu.VMEM((slots, own_rows, total), f32)
    final = jax.ShapeDtypeStruct((slots, own_rows, total), f32)
    stiff, mass = pl.pallas_call(
        functools.partial(kernel, (n, zn, sec, rows, modes, nblk, nband, blk)),
        out_shape=(held, held),
        in_specs=[pl.BlockSpec(memory_space=pltpu.SMEM), hbm, hbm, hbm],
        out_specs=(vmem, vmem),
        scratch_shapes=[
            pltpu.VMEM((CHUNKS, sectors_all, chunk, modes), bf16),
            pltpu.VMEM((slots * cols, n, part, LANES), bf16),
            pltpu.VMEM((slots * cols, rows + 2 * halo, LANES), bf16),
            pltpu.VMEM((total, rows), bf16),
            pltpu.VMEM((rows, wide), bf16),
            pltpu.VMEM((2, nblk, nband, blk, blk), bf16),
            pltpu.VMEM((slots, tiles, LANES, wide), f32),
            pltpu.VMEM((slots, tiles, LANES, wide), bf16),
            pltpu.VMEM((2, slots, tiles, LANES, wide), bf16),
            pltpu.VMEM((slots, tiles, LANES, wide), bf16),
            pltpu.VMEM((slots, cols, own_rows, wide), bf16),
            pltpu.VMEM((slots, cols, LANES, wide), bf16),
            pltpu.VMEM((slots, 2, 2 * n * PACK, sectors_all * PACK), bf16),
            dma((1,)), dma((CHUNKS,)),
            dma((1,)), dma((slots * cols,)), dma((slots * cols,)),
            dma((2,)), dma((slots * cols, 2)),
            dma((2,)), dma((2, slots, tiles)), dma((slots,)),
            dma((2,)), dma((2, slots, cols) if zn != 4 else (2, 1, 1)),
            dma((2,)),
        ],
        compiler_params=pltpu.CompilerParams(
            collective_id=0, has_side_effects=True, vmem_limit_bytes=60000 * 1024),
    )(harmonic_table, psi_sectors, stiff_blocks, mass_blocks)
    return pl.pallas_call(
        flush, out_shape=(final, final), in_specs=[vmem, vmem], out_specs=(hbm, hbm),
        scratch_shapes=[dma((2,))], compiler_params=pltpu.CompilerParams(vmem_limit_bytes=1024 * 1024),
    )(stiff, mass)


def solution(mesh):
    placed = (P("sector", "row", None), P("row", None, None, None), P("row", None, None, None), P())
    return jax.shard_map(
        per_device,
        mesh=mesh,
        in_specs=placed,
        out_specs=(P("sector", "row", None), P("sector", "row", None)),
        check_vma=False,
    )
```
